128 devices in a mesh: pb: 16 (over z, y_hi, core), ka: 8 (over x, y_lo).
Axes of the slice: x: 4, y: 4 (y_hi: 2, y_lo: 2; y = y_hi * 2 + y_lo), z: 4, core: 2. Of those that a mesh axis runs over, the one named last changes fastest.
Arguments:
- activations: bfloat16 [4, 4096, 768], P(None, ('pb', 'ka')), may hold values from -6 to 6
- attn_gain: float32 [768], replicated, may hold values from 0.1 to 1.9
- w_qkv: bfloat16 [768, 2304], replicated, may hold values from -0.21875 to 0.21875
- w_gate: bfloat16 [768, 768], replicated, may hold values from -0.21875 to 0.21875
- w_out: bfloat16 [768, 768], replicated, may hold values from -0.21875 to 0.21875
- pair_bias: bfloat16 [16, 4096, 4096], P(None, 'pb', 'ka'), may hold values from -240 to 240
- chain_ids: int32 [4096], replicated, may hold values from 0 to 5, as said below
- binder_flag: int32 [4096], replicated, may hold values from 0 to 1, as said below
- trans_gain: float32 [768], replicated, may hold values from 0.1 to 1.9
- w_up: bfloat16 [768, 3072], replicated, may hold values from -0.21875 to 0.21875
- w_down: bfloat16 [1536, 768], replicated, may hold values from -0.15625 to 0.15625
Outputs:
- updated: bfloat16 [4, 4096, 768], P(None, ('pb', 'ka'))
The draws below stay inside these ranges and needn't reach their ends.
Inputs may be any that keep to these rules, and one draw needn't show every extreme that they name: `chain_ids`: chain ids never fall along the tokens; every chain has at least one token. `binder_flag`: all tokens of one chain carry the same flag.
All inputs are finite; a program needn't handle non-finite values.
Results may differ from the reference program's by a relative error of at most 0.0056.
Values may be sent and summed in bfloat16 or wider, within the bound.
A program may use at most 128 MiB of HBM per device.

```python
import math
import jax
import jax.numpy as jnp
from jax import lax

D = 768
HEADS = 16
FF = 1536
SAMPLES = 4
CHAINS = 6
TOKENS = 4096
N_PB = 16
N_KA = 8


peak_count = 6


def chain_layout(key):
    cut_key = jax.random.fold_in(key, 11)
    pick_key = jax.random.fold_in(key, 12)
    cut_order = jax.random.permutation(cut_key, TOKENS - 1)[:CHAINS - 1] + 1
    cut_points = jnp.sort(cut_order.astype(jnp.int32))
    positions = jnp.arange(TOKENS, dtype=jnp.int32)
    chain_table = jnp.sum((positions[:, None] >= cut_points[None, :]).astype(jnp.int32), axis=1).astype(jnp.int32)
    chain_picks = jax.random.randint(pick_key, (CHAINS,), 0, 4)
    binder_chain = ((chain_picks == 0) | (jnp.arange(CHAINS, dtype=jnp.int32) == CHAINS - 1)).astype(jnp.int32)
    return (chain_table, binder_chain[chain_table])


def draw_chain_ids(key, part):
    return chain_layout(key)[0]


def draw_binder_flag(key, part):
    return chain_layout(key)[1]


def add_peaks(key, base_bias):
    column_key = jax.random.fold_in(key, 23)
    height_key = jax.random.fold_in(key, 24)
    columns = jax.random.randint(column_key, (HEADS, TOKENS, peak_count), 0, TOKENS)
    heights = jax.random.uniform(height_key, (HEADS, TOKENS, peak_count), jnp.float32, 6.0, 11.0)
    head_index = jnp.broadcast_to(jnp.arange(HEADS, dtype=jnp.int32)[:, None, None], columns.shape)
    row_index = jnp.broadcast_to(jnp.arange(TOKENS, dtype=jnp.int32)[None, :, None], columns.shape)
    return base_bias.at[head_index, row_index, columns].add(heights)


def draw_pair_bias(key, part):
    base_key = jax.random.fold_in(key, 21)
    base_bias = jnp.clip(jax.random.normal(base_key, (HEADS, TOKENS, TOKENS), jnp.float32), -6.0, 6.0)
    return add_peaks(key, base_bias).astype(jnp.bfloat16)


def block_scale(own_key, dims, shards, low, high):
    def one(axis_at, parts):
        steps = jax.random.uniform(jax.random.fold_in(jax.random.fold_in(own_key, 6), axis_at), (parts,), jnp.float32, low / len(shards), high / len(shards))
        return jnp.repeat(jnp.exp(steps), dims[axis_at] // parts).reshape((-1,) + (1,) * (len(dims) - axis_at - 1))

    factor_of = one(*shards[0])
    for cut in shards[1:]:
        factor_of = factor_of * one(*cut)
    return factor_of


def noise(rng, dims, width, limit, cuts=(), kind=jnp.bfloat16):
    array = jax.random.normal(rng, dims, jnp.float32) * width
    if len(cuts) > 0:
        array = block_scale(rng, dims, cuts, -0.22, 0.18) * array
    return jnp.clip(array, min=-limit, max=limit).astype(kind)


def setup_inputs(seed: int = 0) -> dict:
    key_of = jax.random.split(jax.random.key(seed), 12)
    activations = noise(key_of[0], (SAMPLES, TOKENS, D), 1.0, 6.0, ((1, 128),))
    attn_gain = jnp.clip(1.0 + 0.18 * jax.random.normal(key_of[1], (D,), jnp.float32), 0.1, 1.9)
    w_qkv = noise(key_of[2], (D, 3 * D), D ** -0.5, 0.21875)
    w_gate = noise(key_of[3], (D, D), D ** -0.5, 0.21875)
    w_out = noise(key_of[4], (D, D), D ** -0.5, 0.21875)
    pair_bias = draw_pair_bias(jax.random.fold_in(key_of[11], 71), 0)
    chain_ids = draw_chain_ids(jax.random.fold_in(key_of[11], 71), 0)
    binder_flag = draw_binder_flag(jax.random.fold_in(key_of[11], 71), 0)
    trans_gain = jnp.clip(1.0 + 0.18 * jax.random.normal(key_of[8], (D,), jnp.float32), 0.1, 1.9)
    w_up = noise(key_of[9], (D, 2 * FF), D ** -0.5, 0.21875)
    w_down = noise(key_of[10], (FF, D), FF ** -0.5, 0.15625)
    return dict(activations=activations, attn_gain=attn_gain, w_qkv=w_qkv, w_gate=w_gate, w_out=w_out, pair_bias=pair_bias, chain_ids=chain_ids, binder_flag=binder_flag, trans_gain=trans_gain, w_up=w_up, w_down=w_down)


epsilon = 1e-05
masked_score = -1000000000.0

def layer_norm(values, scales):
    centred = values - lax.optimization_barrier(jnp.mean(values, axis=-1, keepdims=True))
    spread = lax.optimization_barrier(jnp.mean(centred * centred, axis=-1, keepdims=True))
    return centred * lax.rsqrt(spread + epsilon) * scales

def widened(values):
    return lax.optimization_barrier(values).astype(jnp.float32)

def block_stats(query_rows, key_block, value_block, bias_tile, allowed):
    head_count = bias_tile.shape[0]
    query_heads = widened(query_rows).reshape(query_rows.shape[0], head_count, -1)
    key_heads = widened(key_block).reshape(key_block.shape[0], head_count, -1)
    value_heads = widened(value_block).reshape(value_block.shape[0], head_count, -1)
    head_size = query_heads.shape[-1]
    scores = jnp.einsum('qhd,khd->hqk', query_heads, key_heads) / math.sqrt(head_size)
    scores = scores + bias_tile.astype(jnp.float32)
    best_score = lax.optimization_barrier(jnp.max(jnp.where(allowed[None], scores, masked_score), axis=-1))
    weights = jnp.where(allowed[None], jnp.exp(scores - best_score[..., None]), 0.0)
    row_sum = lax.optimization_barrier(jnp.sum(weights, axis=-1))
    rounded = widened(weights.astype(jnp.bfloat16))
    block_out = jnp.einsum('hqk,khd->qhd', rounded, value_heads).reshape(query_rows.shape[0], -1)
    return (best_score.T, row_sum.T, block_out)

def reference(activations, attn_gain, w_qkv, w_gate, w_out, pair_bias, chain_ids, binder_flag, trans_gain, w_up, w_down):
    samples, token_count, model_width = activations.shape
    head_count = pair_bias.shape[0]
    normed = layer_norm(activations.astype(jnp.float32), attn_gain).astype(jnp.bfloat16)
    flat_normed = normed.reshape(-1, model_width)
    projected = jnp.dot(flat_normed, w_qkv, preferred_element_type=jnp.float32)
    projected = projected.reshape(samples, token_count, 3 * model_width)
    queries = projected[..., :model_width].astype(jnp.bfloat16)
    key_rows = projected[..., model_width:2 * model_width].astype(jnp.bfloat16)
    value_rows = projected[..., 2 * model_width:].astype(jnp.bfloat16)
    gate_pre = jnp.dot(flat_normed, w_gate, preferred_element_type=jnp.float32)
    gate_pre = gate_pre.reshape(samples, token_count, model_width)
    query_count = token_count // N_PB
    key_count = token_count // N_KA
    stats_per_sample = jax.vmap(block_stats, in_axes=(0, 0, 0, None, None))

    def query_block(block_index):
        start = (block_index * query_count).astype(jnp.int32)
        query_rows = lax.dynamic_slice_in_dim(queries, start, query_count, 1)
        row_chain = lax.dynamic_slice_in_dim(chain_ids, start, query_count, 0)
        row_binder = lax.dynamic_slice_in_dim(binder_flag, start, query_count, 0)
        block_tops, block_sums, block_outs = ([], [], [])
        for key_index in range(N_KA):
            lowest = key_index * key_count
            col_chain = chain_ids[lowest:lowest + key_count]
            col_binder = binder_flag[lowest:lowest + key_count]
            allowed = (row_binder[:, None] > 0) | (col_binder[None, :] > 0) | (row_chain[:, None] == col_chain[None, :])
            bias_tile = lax.dynamic_slice(pair_bias, (jnp.zeros((), jnp.int32), start, jnp.full((), lowest, jnp.int32)), (head_count, query_count, key_count))
            best_score, row_sum, block_out = stats_per_sample(query_rows, key_rows[:, lowest:lowest + key_count], value_rows[:, lowest:lowest + key_count], bias_tile, allowed)
            block_tops.append(best_score)
            block_sums.append(row_sum)
            block_outs.append(block_out)
        block_tops = jnp.stack(block_tops)
        block_sums = jnp.stack(block_sums)
        block_outs = jnp.stack(block_outs)
        overall = lax.optimization_barrier(jnp.max(block_tops, axis=0))
        factors = jnp.exp(block_tops - overall)
        row_sum = lax.optimization_barrier(jnp.sum(factors * block_sums, axis=0))
        shaped = block_outs.reshape(block_outs.shape[:-1] + (head_count, -1))
        summed = lax.optimization_barrier(jnp.sum(factors[..., None] * shaped, axis=0))
        return (summed / row_sum[..., None]).reshape(samples, query_count, model_width)
    attention = lax.map(query_block, jnp.arange(N_PB, dtype=jnp.int32))
    attention = jnp.moveaxis(attention, 0, 1).reshape(samples, token_count, model_width)
    gated = (jax.nn.sigmoid(gate_pre) * attention).astype(jnp.bfloat16)
    mixed = activations.astype(jnp.float32) + jnp.dot(gated.reshape(-1, model_width), w_out, preferred_element_type=jnp.float32).reshape(samples, token_count, model_width)
    trans_normed = layer_norm(mixed, trans_gain).astype(jnp.bfloat16)
    both_parts = jnp.dot(trans_normed.reshape(-1, model_width), w_up, preferred_element_type=jnp.float32)
    hidden_width = w_down.shape[0]
    hidden = (jax.nn.silu(both_parts[:, :hidden_width]) * both_parts[:, hidden_width:]).astype(jnp.bfloat16)
    updated = mixed + jnp.dot(hidden, w_down, preferred_element_type=jnp.float32).reshape(samples, token_count, model_width)
    return updated.astype(jnp.bfloat16)
```

```python
import math

import jax
import jax.numpy as jnp
from jax import lax
from jax.experimental import pallas as pl
from jax.experimental.pallas import tpu as pltpu
from jax.sharding import PartitionSpec as P

EPS = 1e-5
LOG2E = 1.4426950408889634
MASKED = -1e9 * LOG2E
S, ROWS, D, H, HD = 4, 32, 768, 16, 48
NQ, NK, FF = 256, 512, 1536
WIDE = 896
QSCALE = LOG2E / math.sqrt(HD)
BF, F32 = jnp.bfloat16, jnp.float32
MESH = pl.DeviceIdType.MESH


def dot(a, b):
    return jnp.dot(a, b, preferred_element_type=F32)


def dot_t(a, b):
    return lax.dot_general(a, b, (((1,), (1,)), ((), ())), preferred_element_type=F32)


def norm(values, gain):
    centred = values - jnp.mean(values, axis=-1, keepdims=True)
    spread = jnp.mean(centred * centred, axis=-1, keepdims=True)
    return centred * lax.rsqrt(spread + EPS) * gain


def eye(n):
    return (
        lax.broadcasted_iota(jnp.int32, (n, n), 0) == lax.broadcasted_iota(jnp.int32, (n, n), 1)
    ).astype(F32).astype(BF)


def kernel(
    act, gain1, wqkv_h, wgate_h, wout_h, bias_h, chain, binder, gain2, wup_h, wdown_h,
    out,
    xq, xk, rl, wqkv, wgate, wout, wup, wdown, bias, bt, wqt, wvt, wkp, qtp, kp, vt,
    st, ot, lse, msg, rbuf, gate,
    wsem, p1s, p1r, zs, zr, crs, rls, rlr, ds, dr, rss, rsr,
):
    pb, ka = lax.axis_index("pb"), lax.axis_index("ka")
    z, core = pb // 4, pb % 2
    x, ylo = ka // 2, ka % 2
    yhi = (pb // 2) % 2
    r = (z - x + 4) % 4
    same = yhi == ylo
    root = jnp.logical_and(same, r == 0)
    cross0 = jnp.logical_and(jnp.logical_not(same), r == 0)
    cross1 = jnp.logical_and(jnp.logical_not(same), r % 2 == 1)
    not_root = jnp.logical_not(root)
    fwd_a = jnp.logical_and(not_root, r != 3)
    fwd_b = jnp.logical_and(not_root, r != 1)
    side = jnp.where(r == 1, 0, 2)
    xp, xm = (ka + 2) % 8, (ka + 6) % 8
    mate = x * 2 + (1 - ylo)
    zp, zm = (pb + 4) % 16, (pb + 12) % 16
    twin = (pb // 2) * 2 + (1 - core)
    opp = (z * 4 + (1 - yhi) * 2 + core, mate)
    relay_to = jnp.where(r == 1, xp, xm)

    def rcopy(src, dst, ssem, rsem, dev):
        return pltpu.make_async_remote_copy(
            src_ref=src, dst_ref=dst, send_sem=ssem, recv_sem=rsem,
            device_id=dev, device_id_type=MESH,
        )

    local = [
        pltpu.make_async_copy(a, b, wsem.at[i])
        for i, (a, b) in enumerate(
            ((wqkv_h, wqkv), (bias_h, bias), (wgate_h, wgate), (wout_h, wout), (wup_h, wup), (wdown_h, wdown))
        )
    ]
    for c in local:
        c.start()

    for s in range(S):
        xq[s, ka] = norm(act[s].astype(F32), gain1[...]).astype(BF)

    barrier = pltpu.get_barrier_semaphore()
    for i in range(1, 8):
        pl.semaphore_signal(barrier, inc=1, device_id=(pb, (ka + i) % 8), device_id_type=MESH)
    for dev in ((zp, ka), (zm, ka), (twin, ka), opp):
        pl.semaphore_signal(barrier, inc=1, device_id=dev, device_id_type=MESH)
    pl.semaphore_wait(barrier, 11)

    def slice_of(dx, dy):
        y = ylo if dy == 0 else 1 - ylo
        return ((x + dx) % 4) * 2 + y

    def p1(s, n, owner, dev, dx, dy):
        return rcopy(xq.at[s, owner], xq.at[s, owner], p1s.at[s, n], p1r.at[s, dx, dy], dev)

    def own_sends(s):
        return [
            p1(s, 0, ka, (pb, mate), 0, 1),
            p1(s, 1, ka, (pb, xp), 3, 0),
            p1(s, 2, ka, (pb, xm), 1, 0),
        ]

    def mate_sends(s):
        return [
            p1(s, 3, mate, (pb, xp), 3, 1),
            p1(s, 4, mate, (pb, xm), 1, 1),
        ]

    def far_send(s, up):
        if up:
            return p1(s, 5, slice_of(3, 0), (pb, xp), 2, 0)
        return p1(s, 6, slice_of(1, 1), (pb, xm), 2, 1)

    def p1_wait(s, dx, dy):
        o = slice_of(dx, dy)
        rcopy(xq.at[s, o], xq.at[s, o], p1s.at[s, 0], p1r.at[s, dx, dy], (pb, mate)).wait_recv()

    def own(s):
        for c in own_sends(s):
            c.start()

    def pass_on(s):
        p1_wait(s, 0, 1)
        for c in mate_sends(s):
            c.start()
        p1_wait(s, 3, 0)
        far_send(s, True).start()
        p1_wait(s, 1, 1)
        far_send(s, False).start()

    def gathered(s):
        for dx, dy in ((1, 0), (3, 1), (2, 0), (2, 1)):
            p1_wait(s, dx, dy)

    def piece(s, p):
        return xk.at[s, core, pl.ds(2 * p, 2)]

    def root_sends(s):
        cs = []
        for p in range(4):
            cs.append(rcopy(xq.at[s, pl.ds(2 * p, 2)], piece(s, p), zs.at[s, p], zr.at[s, p], (zp if p < 2 else zm, ka)))
        return cs

    def cross_sends(s):
        return [
            rcopy(xq.at[s, pl.ds(2 * p, 2)], piece(s, p), crs.at[s, p // 2], zr.at[s, p], opp) for p in (1, 3)
        ]

    def side_send(s):
        return rcopy(xq.at[s, pl.ds(2 * side, 2)], rl.at[s], crs.at[s, 0], rlr.at[s], opp)

    def relay_send(s):
        return rcopy(rl.at[s], piece(s, side), rls.at[s], zr.at[s, side], (pb, relay_to))

    def pass_send(s, p):
        return rcopy(piece(s, p), piece(s, p), zs.at[s, p], zr.at[s, p], (zp if p < 2 else zm, ka))

    def twin_send(s, src):
        return rcopy(src, xk.at[s, core], ds.at[s], dr.at[s], (twin, ka))

    def roots(s):
        @pl.when(root)
        def _():
            for c in root_sends(s):
                c.start()
            twin_send(s, xq.at[s]).start()
            xk[s, core] = xq[s]

        @pl.when(cross0)
        def _():
            for c in cross_sends(s):
                c.start()

        @pl.when(cross1)
        def _():
            side_send(s).start()

    def relay(s):
        @pl.when(cross1)
        def _():
            rcopy(rl.at[s], rl.at[s], crs.at[s, 0], rlr.at[s], opp).wait_recv()
            relay_send(s).start()

    def spread(s):
        for p in (0, 2, 1, 3):
            @pl.when(not_root)
            def _():
                pass_send(s, p).wait_recv()

            @pl.when(fwd_a if p < 2 else fwd_b)
            def _():
                pass_send(s, p).start()

        @pl.when(not_root)
        def _():
            twin_send(s, xk.at[s, core]).start()

    def prep_weights():
        local[0].wait()
        e = eye(256)
        for i in range(3):
            wqt[256 * i:256 * i + 256, :] = dot_t(e, wqkv[:, 256 * i:256 * i + 256]).astype(BF)
            wvt[256 * i:256 * i + 256, :] = dot_t(e, wqkv[:, 2 * D + 256 * i:2 * D + 256 * i + 256]).astype(BF)
        row = lax.broadcasted_iota(jnp.int32, (256, 256), 0)
        col = lax.broadcasted_iota(jnp.int32, (256, 256), 1)
        source = (col // 64) * HD + col % 64
        for t in range(4):
            start, off = (384 * (t // 2), 0) if t % 2 == 0 else (384 * (t // 2) + 128, 64)
            pick = jnp.logical_and(row == source + off, col % 64 < HD).astype(F32).astype(BF)
            wkp[:, 256 * t:256 * t + 256] = dot(wqkv[:, D + start:D + start + 256], pick).astype(BF)
        qtp[...] = jnp.zeros_like(qtp)
        tail = lax.broadcasted_iota(jnp.int32, (16, 16, NK), 1)
        ot[D + 48:, :] = jnp.zeros((WIDE - D - 48, NQ), BF)
        vt[:, HD:64, :] = (tail == 0).astype(F32).astype(BF)

    def prep_bias():
        local[1].wait()
        qc, qb = chain[pl.ds(pb * 2, 2), :], binder[pl.ds(pb * 2, 2), :]
        kc, kb = chain[pl.ds(ka * 4, 4), :], binder[pl.ds(ka * 4, 4), :]

        def features(c, b, n, at):
            c = jnp.concatenate([c[i:i + 1] for i in range(n // 128)], axis=1)
            b = jnp.concatenate([b[i:i + 1] for i in range(n // 128)], axis=1)
            kind = lax.broadcasted_iota(jnp.int32, (16, n), 0)
            f = jnp.where(kind == c, 1.0, 0.0)
            f = jnp.where(kind == 6 + at, jnp.where(b > 0, 1.0, 0.0), f)
            return jnp.where(kind == 7 - at, 1.0, f).astype(BF)

        allow = lax.dot_general(
            features(kc, kb, NK, 1), features(qc, qb, NQ, 0), (((0,), (0,)), ((), ())), preferred_element_type=F32
        )
        st[0] = allow

        def head(h, carry):
            e = eye(256)
            for t in range(2):
                b = dot_t(e, bias[h, :, 256 * t:256 * t + 256]) * LOG2E
                bt[h, 256 * t:256 * t + 256, :] = jnp.where(st[0, 256 * t:256 * t + 256, :] > 0.5, b, MASKED)
            return carry

        lax.fori_loop(0, H, head, 0)

    def prep_gate():
        local[2].wait()
        n = xq[:, ka].reshape(S * ROWS, D)
        gate[...] = 1.0 / (1.0 + jnp.exp(-dot(n, wgate[...])))

    def attend(s):
        qs = xq[s].reshape(NQ, D)
        q = (dot_t(wqt[...], qs) * QSCALE).astype(BF)
        for h in range(H):
            off = 64 * (h % 2)
            qtp[h, off:off + HD, :] = q[HD * h:HD * h + HD]
        ks = xk[s].reshape(NK, D)
        for n in range(4):
            k = dot(ks, wkp[:, 256 * n:256 * n + 256]).astype(BF)
            kp[2 * n] = k[:, :128]
            kp[2 * n + 1] = k[:, 128:]
        for t in range(2):
            v = dot_t(wvt[...], ks[256 * t:256 * t + 256]).astype(BF)
            for h in range(H):
                vt[h, 0:HD, 256 * t:256 * t + 256] = v[HD * h:HD * h + HD]

        def pair(hp, carry):
            tops = []
            for j in range(2):
                h = 2 * hp + j
                top = None
                for c in range(4):
                    v = dot(kp[hp, 128 * c:128 * c + 128, :], qtp[h]) + bt[h, 128 * c:128 * c + 128, :]
                    st[j, 128 * c:128 * c + 128, :] = v
                    m = jnp.max(v.reshape(16, 8, NQ), axis=0)
                    top = m if top is None else jnp.maximum(top, m)
                tops.append(jnp.max(top, axis=0, keepdims=True))
            for j in range(2):
                h = 2 * hp + j
                w = jnp.exp2(st[j] - tops[j]).astype(BF)
                o = dot(vt[h], w)
                total = o[HD:HD + 1]
                ot[pl.ds(pl.multiple_of(HD * h, 16), HD), :] = (o[:HD] * (1.0 / total)).astype(BF)
                lse[pl.ds(h, 1), :] = tops[j] + jnp.log2(total)
            return carry

        lax.fori_loop(0, H // 2, pair, 0)
        rest = lse[...]
        for i in range(3):
            part = rest.astype(BF)
            ot[D + 16 * i:D + 16 * i + 16, :] = part
            rest = rest - part.astype(F32)
        e = eye(256)
        for t in range(4):
            lo, n = 256 * t, min(256, WIDE - 256 * t)
            msg[s, :, :, lo:lo + n] = dot_t(e, ot[lo:lo + n, :]).astype(BF).reshape(8, ROWS, n)
        rbuf[s, ka] = msg[s, ka]

    def rs_send(s, i):
        to = (ka + i) % 8
        return rcopy(msg.at[s, to], rbuf.at[s, ka], rss.at[s, i - 1], rsr.at[s, 8 - i], (pb, to))

    def rs_wait(s, i):
        frm = (ka + i) % 8
        rcopy(msg.at[s, frm], rbuf.at[s, frm], rss.at[s, 0], rsr.at[s, i], (pb, frm)).wait_recv()

    def finish():
        lane = lax.broadcasted_iota(jnp.int32, (128, 128), 1)
        row = lax.broadcasted_iota(jnp.int32, (128, 128), 0)
        gather = jnp.logical_and(row % 16 == lane % 16, row < 48).astype(F32).astype(BF)
        erow = lax.broadcasted_iota(jnp.int32, (128, D), 0)
        ecol = lax.broadcasted_iota(jnp.int32, (128, D), 1)
        expand = jnp.logical_and(ecol // HD == erow % 16, erow < 32).astype(F32).astype(BF)
        sums = [dot(rbuf[:, b, :, D:].reshape(S * ROWS, 128), gather) for b in range(8)]
        top = sums[0]
        for b in range(1, 8):
            top = jnp.maximum(top, sums[b])
        w = [jnp.exp2(v - top) for v in sums]
        total = w[0]
        for b in range(1, 8):
            total = total + w[b]
        inv = 1.0 / total
        acc = jnp.zeros((S * ROWS, D), F32)
        for b in range(8):
            v = w[b] * inv
            hi = v.astype(BF)
            low = (v - hi.astype(F32)).astype(BF)
            both = jnp.where(lane < 16, hi.astype(F32), jnp.where(lane < 32, low.astype(F32), 0.0)).astype(BF)
            acc = acc + dot(both, expand) * rbuf[:, b, :, :D].reshape(S * ROWS, D).astype(F32)
        gated = (gate[...] * acc).astype(BF)
        local[3].wait()
        mixed = act[...].reshape(S * ROWS, D).astype(F32) + dot(gated, wout[...])
        normed = norm(mixed, gain2[...]).astype(BF)
        local[4].wait()
        left = dot(normed, wup[:, :FF])
        right = dot(normed, wup[:, FF:])
        hidden = (left / (1.0 + jnp.exp(-left)) * right).astype(BF)
        local[5].wait()
        out[...] = (mixed + dot(hidden, wdown[...])).astype(BF).reshape(S, ROWS, D)

    own(0)
    own(1)
    prep_weights()
    pass_on(0)
    own(2)
    pass_on(1)
    own(3)
    gathered(0)
    roots(0)
    prep_bias()
    pass_on(2)
    gathered(1)
    roots(1)
    relay(0)
    pass_on(3)
    gathered(2)
    roots(2)
    relay(1)
    prep_gate()
    gathered(3)
    roots(3)
    relay(2)
    relay(3)
    spread(0)

    def step(s, carry):
        @pl.when(s < S - 1)
        def _():
            spread(s + 1)

        twin_recv(s)
        attend(s)
        for i in (4, 3, 5, 2, 6, 1, 7):
            rs_send(s, i).start()
        return carry

    def twin_recv(s):
        rcopy(xk.at[s, 1 - core], xk.at[s, 1 - core], ds.at[s], dr.at[s], (twin, ka)).wait_recv()

    lax.fori_loop(0, S, step, 0)

    for s in range(S):
        for i in range(1, 8):
            rs_wait(s, i)
    finish()

    for s in range(S):
        for c in own_sends(s) + mate_sends(s) + [far_send(s, True), far_send(s, False)]:
            c.wait_send()
        for i in range(1, 8):
            rs_send(s, i).wait_send()
        twin_send(s, xq.at[s]).wait_send()
        for p in range(4):
            @pl.when(jnp.logical_or(root, fwd_a if p < 2 else fwd_b))
            def _():
                pass_send(s, p).wait_send()

        @pl.when(cross0)
        def _():
            for c in cross_sends(s):
                c.wait_send()

        @pl.when(cross1)
        def _():
            side_send(s).wait_send()
            relay_send(s).wait_send()


def body(act, gain1, wqkv, wgate, wout, bias, chain, binder, gain2, wup, wdown):
    vmem = pl.BlockSpec(memory_space=pltpu.VMEM)
    hbm = pl.BlockSpec(memory_space=pl.ANY)
    dma, v = pltpu.SemaphoreType.DMA, pltpu.VMEM
    return pl.pallas_call(
        kernel,
        out_shape=jax.ShapeDtypeStruct((S, ROWS, D), BF),
        in_specs=[vmem, vmem, hbm, hbm, hbm, hbm, vmem, vmem, vmem, hbm, hbm],
        out_specs=vmem,
        scratch_shapes=[
            v((S, 8, ROWS, D), BF), v((S, 2, 8, ROWS, D), BF), v((S, 2, ROWS, D), BF),
            v((D, 3 * D), BF), v((D, D), BF), v((D, D), BF), v((D, 2 * FF), BF), v((FF, D), BF),
            v((H, NQ, NK), BF), v((H, NK, NQ), F32),
            v((D, D), BF), v((D, D), BF), v((D, 1024), BF),
            v((H, 128, NQ), BF), v((H // 2, NK, 128), BF), v((H, 64, NK), BF),
            v((2, NK, NQ), F32), v((WIDE, NQ), BF), v((H, NQ), F32),
            v((S, 8, ROWS, WIDE), BF), v((S, 8, ROWS, WIDE), BF), v((S * ROWS, D), F32),
            dma((6,)), dma((S, 7)), dma((S, 4, 2)), dma((S, 4)), dma((S, 4)), dma((S, 2)),
            dma((S,)), dma((S,)), dma((S,)), dma((S,)), dma((S, 7)), dma((S, 8)),
        ],
        compiler_params=pltpu.CompilerParams(
            collective_id=0, has_side_effects=True, vmem_limit_bytes=66_000_000
        ),
        name="block",
    )(
        act, gain1.reshape(1, D), wqkv, wgate, wout, bias, chain.reshape(32, 128), binder.reshape(32, 128),
        gain2.reshape(1, D), wup, wdown,
    )


def solution(mesh):
    placed = (
        P(None, ("pb", "ka"), None), P(), P(), P(), P(), P(None, "pb", "ka"), P(), P(), P(), P(), P(),
    )
    return jax.shard_map(
        body, mesh=mesh, in_specs=placed, out_specs=P(None, ("pb", "ka"), None), check_vma=False
    )
```

```python
import math

import jax
import jax.numpy as jnp
from jax import lax
from jax.experimental import pallas as pl
from jax.experimental.pallas import tpu as pltpu
from jax.sharding import PartitionSpec as P

EPS = 1e-5
LOG2E = 1.4426950408889634
MASKED = -1e9 * LOG2E
S, ROWS, D, H, HD = 4, 32, 768, 16, 48
NQ, NK, FF = 256, 512, 1536
WIDE = 896
QSCALE = LOG2E / math.sqrt(HD)
BF, F32 = jnp.bfloat16, jnp.float32
MESH = pl.DeviceIdType.MESH


def dot(a, b):
    return jnp.dot(a, b, preferred_element_type=F32)


def dot_t(a, b):
    return lax.dot_general(a, b, (((1,), (1,)), ((), ())), preferred_element_type=F32)


def norm(values, gain):
    centred = values - jnp.mean(values, axis=-1, keepdims=True)
    spread = jnp.mean(centred * centred, axis=-1, keepdims=True)
    return centred * lax.rsqrt(spread + EPS) * gain


def eye(n):
    return (
        lax.broadcasted_iota(jnp.int32, (n, n), 0) == lax.broadcasted_iota(jnp.int32, (n, n), 1)
    ).astype(F32).astype(BF)


def kernel(
    act, gain1, wqkv_h, wgate_h, wout_h, bias_h, chain, binder, gain2, wup_h, wdown_h,
    out,
    xq, xk, rl, wqkv, wgate, wout, wup, wdown, bias, bt, wqt, wvt, wkp, qtp, kp, vt,
    st, ot, lse, msg, rbuf, gate,
    wsem, p1s, p1r, zs, zr, crs, rls, rlr, ds, dr, rss, rsr,
):
    pb, ka = lax.axis_index("pb"), lax.axis_index("ka")
    z, core = pb // 4, pb % 2
    x, ylo = ka // 2, ka % 2
    yhi = (pb // 2) % 2
    r = (z - x + 4) % 4
    same = yhi == ylo
    root = jnp.logical_and(same, r == 0)
    cross0 = jnp.logical_and(jnp.logical_not(same), r == 0)
    cross1 = jnp.logical_and(jnp.logical_not(same), r % 2 == 1)
    not_root = jnp.logical_not(root)
    fwd_a = jnp.logical_and(not_root, r != 3)
    fwd_b = jnp.logical_and(not_root, r != 1)
    side = jnp.where(r == 1, 1, 3)
    xp, xm = (ka + 2) % 8, (ka + 6) % 8
    mate = x * 2 + (1 - ylo)
    zp, zm = (pb + 4) % 16, (pb + 12) % 16
    twin = (pb // 2) * 2 + (1 - core)
    opp = (z * 4 + (1 - yhi) * 2 + core, mate)
    relay_to = jnp.where(r == 1, xp, xm)

    def rcopy(src, dst, ssem, rsem, dev):
        return pltpu.make_async_remote_copy(
            src_ref=src, dst_ref=dst, send_sem=ssem, recv_sem=rsem,
            device_id=dev, device_id_type=MESH,
        )

    local = [
        pltpu.make_async_copy(a, b, wsem.at[i])
        for i, (a, b) in enumerate(
            ((wqkv_h, wqkv), (bias_h, bias), (wgate_h, wgate), (wout_h, wout), (wup_h, wup), (wdown_h, wdown))
        )
    ]
    for c in local:
        c.start()

    for s in range(S):
        xq[s, ka] = norm(act[s].astype(F32), gain1[...]).astype(BF)

    barrier = pltpu.get_barrier_semaphore()
    for i in range(1, 8):
        pl.semaphore_signal(barrier, inc=1, device_id=(pb, (ka + i) % 8), device_id_type=MESH)
    for dev in ((zp, ka), (zm, ka), (twin, ka), opp):
        pl.semaphore_signal(barrier, inc=1, device_id=dev, device_id_type=MESH)
    pl.semaphore_wait(barrier, 11)

    def slice_of(dx, dy):
        y = ylo if dy == 0 else 1 - ylo
        return ((x + dx) % 4) * 2 + y

    def p1(s, n, owner, dev, dx, dy):
        return rcopy(xq.at[s, owner], xq.at[s, owner], p1s.at[s, n], p1r.at[s, dx, dy], dev)

    def own_sends(s):
        return [
            p1(s, 0, ka, (pb, mate), 0, 1),
            p1(s, 1, ka, (pb, xp), 3, 0),
            p1(s, 2, ka, (pb, xm), 1, 0),
        ]

    def mate_sends(s):
        return [
            p1(s, 3, mate, (pb, xp), 3, 1),
            p1(s, 4, mate, (pb, xm), 1, 1),
        ]

    def far_send(s, up):
        if up:
            return p1(s, 5, slice_of(3, 0), (pb, xp), 2, 0)
        return p1(s, 6, slice_of(1, 1), (pb, xm), 2, 1)

    def p1_wait(s, dx, dy):
        o = slice_of(dx, dy)
        rcopy(xq.at[s, o], xq.at[s, o], p1s.at[s, 0], p1r.at[s, dx, dy], (pb, mate)).wait_recv()

    def own(s):
        for c in own_sends(s):
            c.start()

    def pass_on(s):
        p1_wait(s, 0, 1)
        for c in mate_sends(s):
            c.start()
        p1_wait(s, 3, 0)
        far_send(s, True).start()
        p1_wait(s, 1, 1)
        far_send(s, False).start()

    def gathered(s):
        for dx, dy in ((1, 0), (3, 1), (2, 0), (2, 1)):
            p1_wait(s, dx, dy)

    def piece(s, p):
        return xk.at[s, core, pl.ds(2 * p, 2)]

    def root_sends(s):
        cs = []
        for p in range(4):
            cs.append(rcopy(xq.at[s, pl.ds(2 * p, 2)], piece(s, p), zs.at[s, p], zr.at[s, p], (zp if p < 2 else zm, ka)))
        return cs

    def cross_sends(s):
        return [
            rcopy(xq.at[s, pl.ds(2 * p, 2)], piece(s, p), crs.at[s, p // 2], zr.at[s, p], opp) for p in (0, 2)
        ]

    def side_send(s):
        return rcopy(xq.at[s, pl.ds(2 * side, 2)], rl.at[s], crs.at[s, 0], rlr.at[s], opp)

    def relay_send(s):
        return rcopy(rl.at[s], piece(s, side), rls.at[s], zr.at[s, side], (pb, relay_to))

    def pass_send(s, p):
        return rcopy(piece(s, p), piece(s, p), zs.at[s, p], zr.at[s, p], (zp if p < 2 else zm, ka))

    def twin_send(s, src):
        return rcopy(src, xk.at[s, core], ds.at[s], dr.at[s], (twin, ka))

    def roots(s):
        @pl.when(root)
        def _():
            for c in root_sends(s):
                c.start()
            twin_send(s, xq.at[s]).start()
            xk[s, core] = xq[s]

        @pl.when(cross0)
        def _():
            for c in cross_sends(s):
                c.start()

        @pl.when(cross1)
        def _():
            side_send(s).start()

    def relay(s):
        @pl.when(cross1)
        def _():
            rcopy(rl.at[s], rl.at[s], crs.at[s, 0], rlr.at[s], opp).wait_recv()
            relay_send(s).start()

    def hop(t):
        late = jnp.where(same, 0, 3)
        up = t - 2 * r - late
        down = t - 2 * ((4 - r) % 4) - late

        @pl.when(jnp.logical_and(not_root, jnp.logical_and(up >= 0, up < 2 * S)))
        def _():
            s, p = lax.div(up, 2), lax.rem(up, 2)
            c = rcopy(piece(s, p), piece(s, p), zs.at[s, p], zr.at[s, p], (zp, ka))
            c.wait_recv()

            @pl.when(fwd_a)
            def _():
                c.start()

        @pl.when(jnp.logical_and(not_root, jnp.logical_and(down >= 0, down < 2 * S)))
        def _():
            s, p = lax.div(down, 2), 2 + lax.rem(down, 2)
            c = rcopy(piece(s, p), piece(s, p), zs.at[s, p], zr.at[s, p], (zm, ka))
            c.wait_recv()

            @pl.when(fwd_b)
            def _():
                c.start()

        last = jnp.minimum(up, down)

        @pl.when(jnp.logical_and(not_root, jnp.logical_and(jnp.logical_and(last >= 0, last < 2 * S), lax.rem(last, 2) == 1)))
        def _():
            s = lax.div(last, 2)
            twin_send(s, xk.at[s, core]).start()

    def prep_weights():
        local[0].wait()
        e = eye(256)
        for i in range(3):
            wqt[256 * i:256 * i + 256, :] = dot_t(e, wqkv[:, 256 * i:256 * i + 256]).astype(BF)
            wvt[256 * i:256 * i + 256, :] = dot_t(e, wqkv[:, 2 * D + 256 * i:2 * D + 256 * i + 256]).astype(BF)
        row = lax.broadcasted_iota(jnp.int32, (256, 256), 0)
        col = lax.broadcasted_iota(jnp.int32, (256, 256), 1)
        source = (col // 64) * HD + col % 64
        for t in range(4):
            start, off = (384 * (t // 2), 0) if t % 2 == 0 else (384 * (t // 2) + 128, 64)
            pick = jnp.logical_and(row == source + off, col % 64 < HD).astype(F32).astype(BF)
            wkp[:, 256 * t:256 * t + 256] = dot(wqkv[:, D + start:D + start + 256], pick).astype(BF)
        qtp[...] = jnp.zeros_like(qtp)
        tail = lax.broadcasted_iota(jnp.int32, (16, 16, NK), 1)
        ot[D + 48:, :] = jnp.zeros((WIDE - D - 48, NQ), BF)
        vt[:, HD:64, :] = (tail == 0).astype(F32).astype(BF)

    def prep_bias():
        local[1].wait()
        qc, qb = chain[pl.ds(pb * 2, 2), :], binder[pl.ds(pb * 2, 2), :]
        kc, kb = chain[pl.ds(ka * 4, 4), :], binder[pl.ds(ka * 4, 4), :]

        def features(c, b, n, at):
            c = jnp.concatenate([c[i:i + 1] for i in range(n // 128)], axis=1)
            b = jnp.concatenate([b[i:i + 1] for i in range(n // 128)], axis=1)
            kind = lax.broadcasted_iota(jnp.int32, (16, n), 0)
            f = jnp.where(kind == c, 1.0, 0.0)
            f = jnp.where(kind == 6 + at, jnp.where(b > 0, 1.0, 0.0), f)
            return jnp.where(kind == 7 - at, 1.0, f).astype(BF)

        allow = lax.dot_general(
            features(kc, kb, NK, 1), features(qc, qb, NQ, 0), (((0,), (0,)), ((), ())), preferred_element_type=F32
        )
        st[0] = allow

        def head(h, carry):
            e = eye(256)
            for t in range(2):
                b = dot_t(e, bias[h, :, 256 * t:256 * t + 256]) * LOG2E
                bt[h, 256 * t:256 * t + 256, :] = jnp.where(st[0, 256 * t:256 * t + 256, :] > 0.5, b, MASKED)
            return carry

        lax.fori_loop(0, H, head, 0)

    def prep_gate():
        local[2].wait()
        n = xq[:, ka].reshape(S * ROWS, D)
        gate[...] = 1.0 / (1.0 + jnp.exp(-dot(n, wgate[...])))

    def attend(s):
        qs = xq[s].reshape(NQ, D)
        q = (dot_t(wqt[...], qs) * QSCALE).astype(BF)
        for h in range(H):
            off = 64 * (h % 2)
            qtp[h, off:off + HD, :] = q[HD * h:HD * h + HD]
        ks = xk[s].reshape(NK, D)
        for n in range(4):
            k = dot(ks, wkp[:, 256 * n:256 * n + 256]).astype(BF)
            kp[2 * n] = k[:, :128]
            kp[2 * n + 1] = k[:, 128:]
        for t in range(2):
            v = dot_t(wvt[...], ks[256 * t:256 * t + 256]).astype(BF)
            for h in range(H):
                vt[h, 0:HD, 256 * t:256 * t + 256] = v[HD * h:HD * h + HD]

        def pair(hp, carry):
            @pl.when(jnp.logical_and(s < S - 1, hp % 4 == 2))
            def _():
                hop(11 + 2 * s + hp // 4)

            tops = []
            for j in range(2):
                h = 2 * hp + j
                top = None
                for c in range(4):
                    v = dot(kp[hp, 128 * c:128 * c + 128, :], qtp[h]) + bt[h, 128 * c:128 * c + 128, :]
                    st[j, 128 * c:128 * c + 128, :] = v
                    m = jnp.max(v.reshape(16, 8, NQ), axis=0)
                    top = m if top is None else jnp.maximum(top, m)
                tops.append(jnp.max(top, axis=0, keepdims=True))
            for j in range(2):
                h = 2 * hp + j
                w = jnp.exp2(st[j] - tops[j]).astype(BF)
                o = dot(vt[h], w)
                total = o[HD:HD + 1]
                ot[pl.ds(pl.multiple_of(HD * h, 16), HD), :] = (o[:HD] * (1.0 / total)).astype(BF)
                lse[pl.ds(h, 1), :] = tops[j] + jnp.log2(total)
            return carry

        lax.fori_loop(0, H // 2, pair, 0)
        rest = lse[...]
        for i in range(3):
            part = rest.astype(BF)
            ot[D + 16 * i:D + 16 * i + 16, :] = part
            rest = rest - part.astype(F32)
        e = eye(256)
        for t in range(4):
            lo, n = 256 * t, min(256, WIDE - 256 * t)
            msg[s, :, :, lo:lo + n] = dot_t(e, ot[lo:lo + n, :]).astype(BF).reshape(8, ROWS, n)
        rbuf[s, ka] = msg[s, ka]

    def rs_send(s, i):
        to = (ka + i) % 8
        return rcopy(msg.at[s, to], rbuf.at[s, ka], rss.at[s, i - 1], rsr.at[s, 8 - i], (pb, to))

    def rs_wait(s, i):
        frm = (ka + i) % 8
        rcopy(msg.at[s, frm], rbuf.at[s, frm], rss.at[s, 0], rsr.at[s, i], (pb, frm)).wait_recv()

    def finish():
        lane = lax.broadcasted_iota(jnp.int32, (128, 128), 1)
        row = lax.broadcasted_iota(jnp.int32, (128, 128), 0)
        gather = jnp.logical_and(row % 16 == lane % 16, row < 48).astype(F32).astype(BF)
        erow = lax.broadcasted_iota(jnp.int32, (128, D), 0)
        ecol = lax.broadcasted_iota(jnp.int32, (128, D), 1)
        expand = jnp.logical_and(ecol // HD == erow % 16, erow < 32).astype(F32).astype(BF)
        sums = [dot(rbuf[:, b, :, D:].reshape(S * ROWS, 128), gather) for b in range(8)]
        top = sums[0]
        for b in range(1, 8):
            top = jnp.maximum(top, sums[b])
        w = [jnp.exp2(v - top) for v in sums]
        total = w[0]
        for b in range(1, 8):
            total = total + w[b]
        inv = 1.0 / total
        acc = jnp.zeros((S * ROWS, D), F32)
        for b in range(8):
            v = w[b] * inv
            hi = v.astype(BF)
            low = (v - hi.astype(F32)).astype(BF)
            both = jnp.where(lane < 16, hi.astype(F32), jnp.where(lane < 32, low.astype(F32), 0.0)).astype(BF)
            acc = acc + dot(both, expand) * rbuf[:, b, :, :D].reshape(S * ROWS, D).astype(F32)
        gated = (gate[...] * acc).astype(BF)
        local[3].wait()
        mixed = act[...].reshape(S * ROWS, D).astype(F32) + dot(gated, wout[...])
        normed = norm(mixed, gain2[...]).astype(BF)
        local[4].wait()
        left = dot(normed, wup[:, :FF])
        right = dot(normed, wup[:, FF:])
        hidden = (left / (1.0 + jnp.exp(-left)) * right).astype(BF)
        local[5].wait()
        out[...] = (mixed + dot(hidden, wdown[...])).astype(BF).reshape(S, ROWS, D)

    own(0)
    own(1)
    prep_weights()
    pass_on(0)
    own(2)
    pass_on(1)
    own(3)
    gathered(0)
    roots(0)
    prep_bias()
    pass_on(2)
    gathered(1)
    roots(1)
    relay(0)
    for t in range(4):
        hop(t)
    pass_on(3)
    gathered(2)
    roots(2)
    relay(1)
    for t in range(4, 6):
        hop(t)
    prep_gate()
    gathered(3)
    roots(3)
    relay(2)
    for t in range(6, 8):
        hop(t)
    relay(3)
    for t in range(8, 11):
        hop(t)

    def step(s, carry):
        twin_recv(s)
        attend(s)
        for i in (4, 3, 5, 2, 6, 1, 7):
            rs_send(s, i).start()
        return carry

    def twin_recv(s):
        rcopy(xk.at[s, 1 - core], xk.at[s, 1 - core], ds.at[s], dr.at[s], (twin, ka)).wait_recv()

    lax.fori_loop(0, S, step, 0)

    for s in range(S):
        for i in range(1, 8):
            rs_wait(s, i)
    finish()

    for s in range(S):
        for c in own_sends(s) + mate_sends(s) + [far_send(s, True), far_send(s, False)]:
            c.wait_send()
        for i in range(1, 8):
            rs_send(s, i).wait_send()
        twin_send(s, xq.at[s]).wait_send()
        for p in range(4):
            @pl.when(jnp.logical_or(root, fwd_a if p < 2 else fwd_b))
            def _():
                pass_send(s, p).wait_send()

        @pl.when(cross0)
        def _():
            for c in cross_sends(s):
                c.wait_send()

        @pl.when(cross1)
        def _():
            side_send(s).wait_send()
            relay_send(s).wait_send()


def body(act, gain1, wqkv, wgate, wout, bias, chain, binder, gain2, wup, wdown):
    vmem = pl.BlockSpec(memory_space=pltpu.VMEM)
    hbm = pl.BlockSpec(memory_space=pl.ANY)
    dma, v = pltpu.SemaphoreType.DMA, pltpu.VMEM
    return pl.pallas_call(
        kernel,
        out_shape=jax.ShapeDtypeStruct((S, ROWS, D), BF),
        in_specs=[vmem, vmem, hbm, hbm, hbm, hbm, vmem, vmem, vmem, hbm, hbm],
        out_specs=vmem,
        scratch_shapes=[
            v((S, 8, ROWS, D), BF), v((S, 2, 8, ROWS, D), BF), v((S, 2, ROWS, D), BF),
            v((D, 3 * D), BF), v((D, D), BF), v((D, D), BF), v((D, 2 * FF), BF), v((FF, D), BF),
            v((H, NQ, NK), BF), v((H, NK, NQ), F32),
            v((D, D), BF), v((D, D), BF), v((D, 1024), BF),
            v((H, 128, NQ), BF), v((H // 2, NK, 128), BF), v((H, 64, NK), BF),
            v((2, NK, NQ), F32), v((WIDE, NQ), BF), v((H, NQ), F32),
            v((S, 8, ROWS, WIDE), BF), v((S, 8, ROWS, WIDE), BF), v((S * ROWS, D), F32),
            dma((6,)), dma((S, 7)), dma((S, 4, 2)), dma((S, 4)), dma((S, 4)), dma((S, 2)),
            dma((S,)), dma((S,)), dma((S,)), dma((S,)), dma((S, 7)), dma((S, 8)),
        ],
        compiler_params=pltpu.CompilerParams(
            collective_id=0, has_side_effects=True, vmem_limit_bytes=66_000_000
        ),
        name="block",
    )(
        act, gain1.reshape(1, D), wqkv, wgate, wout, bias, chain.reshape(32, 128), binder.reshape(32, 128),
        gain2.reshape(1, D), wup, wdown,
    )


def solution(mesh):
    placed = (
        P(None, ("pb", "ka"), None), P(), P(), P(), P(), P(None, "pb", "ka"), P(), P(), P(), P(), P(),
    )
    return jax.shard_map(
        body, mesh=mesh, in_specs=placed, out_specs=P(None, ("pb", "ka"), None), check_vma=False
    )
```

```python
import math

import jax
import jax.numpy as jnp
from jax import lax
from jax.experimental import pallas as pl
from jax.experimental.pallas import tpu as pltpu
from jax.sharding import PartitionSpec as P

EPS = 1e-5
LOG2E = 1.4426950408889634
MASKED = -1e9 * LOG2E
S, ROWS, D, H, HD = 4, 32, 768, 16, 48
NQ, NK, FF = 256, 512, 1536
QSCALE = LOG2E / math.sqrt(HD)
BF, F32 = jnp.bfloat16, jnp.float32
MESH = pl.DeviceIdType.MESH


def dot(a, b):
    return jnp.dot(a, b, preferred_element_type=F32)


def dot_t(a, b):
    return lax.dot_general(a, b, (((1,), (1,)), ((), ())), preferred_element_type=F32)


def norm(values, gain):
    centred = values - jnp.mean(values, axis=-1, keepdims=True)
    spread = jnp.mean(centred * centred, axis=-1, keepdims=True)
    return centred * lax.rsqrt(spread + EPS) * gain


def eye(n):
    return (
        lax.broadcasted_iota(jnp.int32, (n, n), 0) == lax.broadcasted_iota(jnp.int32, (n, n), 1)
    ).astype(F32).astype(BF)


UP = ((0, 0), (1, 0), (1, 1), (2, 0))
DOWN = ((0, 1), (3, 0), (3, 1), (2, 1))
CLASSES = [(e, r) for e in (1, 0) for r in range(4)]


def slot(dx, dy):
    return UP.index((dx, dy)) if (dx, dy) in UP else 4 + DOWN.index((dx, dy))


def rank(op):
    s, kind = op[1], op[0]
    if kind in ("own", "mate", "far", "relay"):
        return s + ("own", "mate", "far", "relay").index(kind)
    return 10 * s + (op[3] if kind == "z" else op[2])


def traffic(occupied=23, latency=44):
    have = {c: {} for c in CLASSES}
    pend, free, log = {}, {}, {c: [] for c in CLASSES}
    for c in CLASSES:
        e, r = c
        ops = {l: [] for l in ("x+", "x-", "y", "o", "z+", "z-")}
        for s in range(S):
            have[c]["q", s, 0, 0] = 0
            ops["y"].append((("own", s), ("q", s, 0, 0)))
            for d in ("x+", "x-"):
                ops[d].append((("own", s), ("q", s, 0, 0)))
                ops[d].append((("mate", s), ("q", s, 0, 1)))
            ops["x+"].append((("far", s), ("q", s, 3, 0)))
            ops["x-"].append((("far", s), ("q", s, 1, 1)))
            for d, owners, end in (("z+", UP, 3), ("z-", DOWN, 1)):
                for g in range(4):
                    if r != end:
                        ops[d].append((("z", s, d, g), ("q" if c == (1, 0) else "k", s) + owners[g]))
            if c == (0, 0):
                ops["o"] += [(("cross", s, dx, dy), ("q", s, dx, dy)) for dx in (0, 2) for dy in (0, 1)]
            if e == 0 and r in (1, 3):
                for dy in (0, 1):
                    ops["o"].append((("side", s, dy), ("q", s, 0, dy)))
                    ops["x+" if r == 1 else "x-"].append((("relay", s, dy), ("rl", s, dy)))
        pend[c] = ops
        free.update({(c, l): 0 for l in ops})
    for now in range(2000):
        for c in CLASSES:
            e, r = c
            for l, ops in pend[c].items():
                ready = [o for o in ops if have[c].get(o[1], now + 1) <= now]
                if free[c, l] > now or not ready:
                    continue
                o = min(ready, key=lambda o: rank(o[0]))
                ops.remove(o)
                free[c, l] = now + occupied
                op, s = o[0], o[0][1]
                log[c].append((now, op, o[1], l))
                step = {"x+": -1, "x-": 1, "z+": 1, "z-": -1}.get(l, 0)
                to = (1 - e if l == "y" else e, (r + step) % 4)
                if op[0] == "z":
                    item = ("k",) + o[1][1:]
                elif op[0] == "cross":
                    item = ("k",) + op[1:]
                elif op[0] == "side":
                    item = ("rl",) + op[1:]
                elif op[0] == "relay":
                    item = ("k", s, 3 if r == 1 else 1, op[2])
                elif l == "y":
                    item = ("q", s, 0, 1)
                elif op[0] == "far":
                    item = ("q", s, 2, 0 if l == "x+" else 1)
                else:
                    item = ("q", s, 3 if l == "x+" else 1, 0 if op[0] == "own" else 1)
                assert item not in have[to]
                have[to][item] = now + occupied + latency
    plans = {}
    for c in CLASSES:
        assert not any(pend[c].values())
        events = [(t, ("send",) + tuple(rest)) for t, *rest in log[c]]
        for s in range(S):
            for kind in ("q", "k"):
                items = [(kind, s, dx, dy) for dx in range(4) for dy in range(2)]
                if kind == "k" and c == (1, 0):
                    continue
                at = max(have[c][i] for i in items)
                events.append((at, ("all", kind, s, items)))
                if kind == "k" or c == (1, 0):
                    events.append((at, ("twin", s)))
        events.sort(key=lambda v: v[0])
        waited = {("q", s, 0, 0) for s in range(S)}
        plan = []
        for at, ev in events:
            needs = ev[3] if ev[0] == "all" else [ev[2]] if ev[0] == "send" else []
            for item in needs:
                if item not in waited:
                    waited.add(item)
                    plan.append((at, ("wait", item)))
            if ev[0] != "all":
                plan.append((at, ev))
        plans[c] = plan
    return plans


def kernel(
    act, gain1, wqkv_h, wgate_h, wout_h, bias_h, chain, binder, gain2, wup_h, wdown_h,
    out,
    xq, xk, rl, wqkv, wgate, wout, wup, wdown, bias, bt, wqt, wvt, wkp, qtp, kp, vt,
    st, ot, lse, msg, rbuf, smsg, srbuf, ost, gate,
    wsem, p1s, p1r, zs, zr, crs, rls, rlr, ds, dr, rss, rsr, sss, ssr,
):
    pb, ka = lax.axis_index("pb"), lax.axis_index("ka")
    z, core = pb // 4, pb % 2
    x, ylo = ka // 2, ka % 2
    yhi = (pb // 2) % 2
    r = (z - x + 4) % 4
    same = yhi == ylo
    odd = jnp.where(same, 0, 1)
    xp, xm = (ka + 2) % 8, (ka + 6) % 8
    mate = x * 2 + (1 - ylo)
    zp, zm = (pb + 4) % 16, (pb + 12) % 16
    twin = (pb // 2) * 2 + (1 - core)
    opp = (z * 4 + (1 - yhi) * 2 + core, mate)

    def rcopy(src, dst, ssem, rsem, dev):
        return pltpu.make_async_remote_copy(
            src_ref=src, dst_ref=dst, send_sem=ssem, recv_sem=rsem,
            device_id=dev, device_id_type=MESH,
        )

    local = [
        pltpu.make_async_copy(a, b, wsem.at[i])
        for i, (a, b) in enumerate(
            ((wqkv_h, wqkv), (bias_h, bias), (wgate_h, wgate), (wout_h, wout), (wup_h, wup), (wdown_h, wdown))
        )
    ]
    for c in local:
        c.start()

    barrier = pltpu.get_barrier_semaphore()
    for i in range(1, 8):
        pl.semaphore_signal(barrier, inc=1, device_id=(pb, (ka + i) % 8), device_id_type=MESH)
    for dev in ((zp, ka), (zm, ka), (twin, ka), opp):
        pl.semaphore_signal(barrier, inc=1, device_id=dev, device_id_type=MESH)

    for s in range(S):
        xq[s, ka] = norm(act[s].astype(F32), gain1[...].reshape(1, D)).astype(BF)

    pl.semaphore_wait(barrier, 11)

    def q_at(dx, dy):
        return ((x + dx) % 4) * 2 + (ylo + dy) % 2

    def k_at(dx, dy):
        return ((x + dx) % 4) * 2 + (ylo + dy + odd) % 2

    def sent(c, op, item, link):
        kind, s = op[0], op[1]
        if kind in ("own", "mate", "far"):
            ref = xq.at[s, q_at(*item[2:])]
            up = link == "x+"
            if link == "y":
                n, sem, to = 0, (0, 1), mate
            else:
                to = xp if up else xm
                n = {"own": 1, "mate": 3, "far": 5}[kind] + (0 if up else 1)
                if kind == "far":
                    sem = (2, 0 if up else 1)
                else:
                    sem = (3 if up else 1, 0 if kind == "own" else 1)
            return rcopy(ref, ref, p1s.at[s, n], p1r.at[s, sem[0], sem[1]], (pb, to))
        if kind == "z":
            owner = item[2:]
            at = k_at(*owner)
            n = slot(*owner)
            src = xq if item[0] == "q" else xk.at[:, core]
            return rcopy(src.at[s, at], xk.at[s, core, at], zs.at[s, n], zr.at[s, n], (zp if link == "z+" else zm, ka))
        if kind == "cross":
            at = q_at(*item[2:])
            return rcopy(xq.at[s, at], xk.at[s, core, at], crs.at[s, op[2] + op[3]], zr.at[s, slot(*item[2:])], opp)
        dy = op[2]
        if kind == "side":
            return rcopy(xq.at[s, q_at(0, dy)], rl.at[s, dy], crs.at[s, dy], rlr.at[s, dy], opp)
        n = slot(3 if c[1] == 1 else 1, dy)
        return rcopy(rl.at[s, dy], xk.at[s, core, k_at(0, dy)], rls.at[s, dy], zr.at[s, n], (pb, xp if c[1] == 1 else xm))

    def arrived(item):
        s = item[1]
        if item[0] == "q":
            ref, ssem, rsem = xq.at[s, q_at(*item[2:])], p1s.at[s, 0], p1r.at[s, item[2], item[3]]
        elif item[0] == "k":
            n = slot(*item[2:])
            ref, ssem, rsem = xk.at[s, core, k_at(*item[2:])], zs.at[s, n], zr.at[s, n]
        else:
            ref, ssem, rsem = rl.at[s, item[2]], rls.at[s, item[2]], rlr.at[s, item[2]]
        rcopy(ref, ref, ssem, rsem, opp).wait_recv()

    def twin_send(s, src):
        return rcopy(src, xk.at[s, core], ds.at[s], dr.at[s], (twin, ka))

    plans = traffic()

    def each_class(body):
        for c in CLASSES:
            @pl.when(jnp.logical_and(odd == 1 - c[0], r == c[1]))
            def _():
                body(c)

    done = [0]

    def until(us):
        low, high = done[0], int(us * 20)
        done[0] = high
        for c in CLASSES:
            events = [ev for at, ev in plans[c] if low <= at < high]
            if not events:
                continue

            @pl.when(jnp.logical_and(odd == 1 - c[0], r == c[1]))
            def _():
                for ev in events:
                    if ev[0] == "wait":
                        arrived(ev[1])
                    elif ev[0] == "send":
                        sent(c, *ev[1:]).start()
                    elif c == (1, 0):
                        twin_send(ev[1], xq.at[ev[1]]).start()
                        xk[ev[1], core] = xq[ev[1]]
                    else:
                        twin_send(ev[1], xk.at[ev[1], core]).start()

    def turn_query_weights():
        local[0].wait()
        e = eye(256)
        for i in range(3):
            wqt[256 * i:256 * i + 256, :] = dot_t(e, wqkv[:, 256 * i:256 * i + 256]).astype(BF)
        qtp[...] = jnp.zeros_like(qtp)

    def turn_value_weights():
        e = eye(256)
        for i in range(3):
            wvt[256 * i:256 * i + 256, :] = dot_t(e, wqkv[:, 2 * D + 256 * i:2 * D + 256 * i + 256]).astype(BF)
        ost[...] = jnp.zeros_like(ost)
        tail = lax.broadcasted_iota(jnp.int32, (16, 16, NK), 1)
        vt[:, HD:64, :] = (tail == 0).astype(F32).astype(BF)

    def pad_key_weights():
        row = lax.broadcasted_iota(jnp.int32, (256, 256), 0)
        col = lax.broadcasted_iota(jnp.int32, (256, 256), 1)
        source = (col // 64) * HD + col % 64
        for t in range(4):
            start, off = (384 * (t // 2), 0) if t % 2 == 0 else (384 * (t // 2) + 128, 64)
            pick = jnp.logical_and(row == source + off, col % 64 < HD).astype(F32).astype(BF)
            wkp[:, 256 * t:256 * t + 256] = dot(wqkv[:, D + start:D + start + 256], pick).astype(BF)

    def prep_bias():
        local[1].wait()
        qc, qb = chain[pl.ds(pb * 2, 2), :], binder[pl.ds(pb * 2, 2), :]
        kc, kb = chain[pl.ds(ka * 4, 4), :], binder[pl.ds(ka * 4, 4), :]

        def features(c, b, n, at):
            c = jnp.concatenate([c[i:i + 1] for i in range(n // 128)], axis=1)
            b = jnp.concatenate([b[i:i + 1] for i in range(n // 128)], axis=1)
            kind = lax.broadcasted_iota(jnp.int32, (16, n), 0)
            f = jnp.where(kind == c, 1.0, 0.0)
            f = jnp.where(kind == 6 + at, jnp.where(b > 0, 1.0, 0.0), f)
            return jnp.where(kind == 7 - at, 1.0, f).astype(BF)

        allow = lax.dot_general(
            features(kc, kb, NK, 1), features(qc, qb, NQ, 0), (((0,), (0,)), ((), ())), preferred_element_type=F32
        )
        st[0, 0] = allow

    def bias_part(i):
        def head(h, carry):
            e = eye(256)
            for t in range(2):
                b = dot_t(e, bias[h, :, 256 * t:256 * t + 256]) * LOG2E
                bt[h, 256 * t:256 * t + 256, :] = jnp.where(st[0, 0, 256 * t:256 * t + 256, :] > 0.5, b, MASKED)
            return carry

        lax.fori_loop(2 * i, 2 * i + 2, head, 0)

    def prep_gate():
        local[2].wait()
        n = xq[:, ka].reshape(S * ROWS, D)
        gate[...] = 1.0 / (1.0 + jnp.exp(-dot(n, wgate[...])))

    def queries(s):
        qs = xq[s].reshape(NQ, D)
        q = (dot_t(wqt[...], qs) * QSCALE).astype(BF)
        for h in range(H):
            off = 64 * (h % 2)
            qtp[s, h, off:off + HD, :] = q[HD * h:HD * h + HD]

    inner = (27.5, 29, 30.5, 32, 34, 35.5, 37, 38.5, 90)

    def window(i, n):
        at = 3 * i + n
        done[0] = int(20 * (inner[at - 1] if at else outer))
        until(inner[at])

    def attend(s):
        ks = xk[s].reshape(NK, D)
        for n in range(4):
            k = dot(ks, wkp[:, 256 * n:256 * n + 256]).astype(BF)
            kp[2 * n] = k[:, :128]
            kp[2 * n + 1] = k[:, 128:]
        for t in range(2):
            v = dot_t(wvt[...], ks[256 * t:256 * t + 256]).astype(BF)
            for h in range(H):
                vt[h, 0:HD, 256 * t:256 * t + 256] = v[HD * h:HD * h + HD]

        def scores(hp):
            tops = []
            for j in range(2):
                h = 2 * hp + j
                top = None
                for c in range(4):
                    v = dot(kp[hp, 128 * c:128 * c + 128, :], qtp[s, h]) + bt[h, 128 * c:128 * c + 128, :]
                    st[hp % 2, j, 128 * c:128 * c + 128, :] = v
                    m = jnp.max(v.reshape(16, 8, NQ), axis=0)
                    top = m if top is None else jnp.maximum(top, m)
                tops.append(jnp.max(top, axis=0, keepdims=True))
            return tops

        def weigh(hp, tops):
            for j in range(2):
                h = 2 * hp + j
                w = jnp.exp2(st[hp % 2, j] - tops[j]).astype(BF)
                o = dot(vt[h], w)
                total = o[HD:HD + 1]
                ot[HD * h:HD * h + HD, :] = (o[:HD] * (1.0 / total)).astype(BF)
                lse[h:h + 1, :] = tops[j] + jnp.log2(total)

        tops = scores(0)
        for hp in range(H // 2):
            if hp in (0, 2, 5):
                for i in range(S - 1):
                    @pl.when(s == i)
                    def _():
                        window(i, (0, 2, 5).index(hp))

            later = scores(hp + 1) if hp < H // 2 - 1 else None
            weigh(hp, tops)
            tops = later
        rest = lse[...]
        for i in range(2):
            part = rest.astype(BF)
            ost[pl.ds(pl.multiple_of(32 * s + 16 * i, 16), 16), :] = part
            rest = rest - part.astype(F32)
        e = eye(256)
        for t in range(3):
            lo = 256 * t
            msg[s, :, :, lo:lo + 256] = dot_t(e, ot[lo:lo + 256, :]).astype(BF).reshape(8, ROWS, 256)
        rbuf[s, ka] = msg[s, ka]

    def rs_send(s, i):
        to = (ka + i) % 8
        return rcopy(msg.at[s, to], rbuf.at[s, ka], rss.at[s, i - 1], rsr.at[s, 8 - i], (pb, to))

    def rs_wait(s, i):
        frm = (ka + i) % 8
        rcopy(msg.at[s, frm], rbuf.at[s, frm], rss.at[s, 0], rsr.at[s, i], (pb, frm)).wait_recv()

    def stat_send(i):
        to = (ka + i) % 8
        return rcopy(smsg.at[to], srbuf.at[ka], sss.at[i - 1], ssr.at[8 - i], (pb, to))

    def stat_wait(i):
        frm = (ka + i) % 8
        rcopy(smsg.at[frm], srbuf.at[frm], sss.at[0], ssr.at[i], (pb, frm)).wait_recv()

    def stats():
        smsg[...] = dot_t(eye(256), ost[...]).astype(BF).reshape(8, ROWS, 128)
        srbuf[ka] = smsg[ka]

    def finish():
        lane = lax.broadcasted_iota(jnp.int32, (128, 128), 1)
        row = lax.broadcasted_iota(jnp.int32, (128, 128), 0)
        erow = lax.broadcasted_iota(jnp.int32, (128, D), 0)
        ecol = lax.broadcasted_iota(jnp.int32, (128, D), 1)
        expand = jnp.logical_and(ecol // HD == erow % 16, erow < 32).astype(F32).astype(BF)
        parts = srbuf[...].reshape(8 * ROWS, 128)
        logs = []
        for s in range(S):
            own = jnp.logical_and(row % 16 == lane % 16, row // 32 == s).astype(F32).astype(BF)
            logs.append(dot(parts, own))
        sums = [jnp.concatenate([v[ROWS * b:ROWS * b + ROWS] for v in logs], axis=0) for b in range(8)]
        top = sums[0]
        for b in range(1, 8):
            top = jnp.maximum(top, sums[b])
        w = [jnp.exp2(v - top) for v in sums]
        total = w[0]
        for b in range(1, 8):
            total = total + w[b]
        inv = 1.0 / total
        acc = jnp.zeros((S * ROWS, D), F32)
        for b in range(8):
            v = w[b] * inv
            hi = v.astype(BF)
            low = (v - hi.astype(F32)).astype(BF)
            both = jnp.where(lane < 16, hi.astype(F32), jnp.where(lane < 32, low.astype(F32), 0.0)).astype(BF)
            acc = acc + dot(both, expand) * rbuf[:, b].reshape(S * ROWS, D).astype(F32)
        gated = (gate[...] * acc).astype(BF)
        local[3].wait()
        mixed = act[...].reshape(S * ROWS, D).astype(F32) + dot(gated, wout[...])
        normed = norm(mixed, gain2[...].reshape(1, D)).astype(BF)
        local[4].wait()
        left = dot(normed, wup[:, :FF])
        right = dot(normed, wup[:, FF:])
        hidden = (left / (1.0 + jnp.exp(-left)) * right).astype(BF)
        local[5].wait()
        out[...] = (mixed + dot(hidden, wdown[...])).astype(BF).reshape(S, ROWS, D)

    until(1)
    turn_query_weights()
    until(3.4)
    turn_value_weights()
    until(4)
    pad_key_weights()
    until(5)
    prep_bias()
    until(6)
    for i in range(8):
        bias_part(i)
        until(7 + i)
    queries(0)
    until(15)
    prep_gate()
    until(16)
    queries(1)
    for us in (17, 18, 19, 20):
        until(us)
    queries(2)
    for us in (21, 22, 23):
        until(us)
    outer = 25.5
    until(outer)
    queries(3)

    def step(s, carry):
        twin_recv(s)
        attend(s)
        for i in (4, 3, 5, 2, 6, 1, 7):
            rs_send(s, i).start()
        return carry

    def twin_recv(s):
        rcopy(xk.at[s, 1 - core], xk.at[s, 1 - core], ds.at[s], dr.at[s], (twin, ka)).wait_recv()

    lax.fori_loop(0, S, step, 0)

    stats()
    for i in (4, 3, 5, 2, 6, 1, 7):
        stat_send(i).start()
    for s in range(S):
        for i in range(1, 8):
            rs_wait(s, i)
    for i in range(1, 8):
        stat_wait(i)
    finish()

    for s in range(S):
        for i in range(1, 8):
            rs_send(s, i).wait_send()
        twin_send(s, xq.at[s]).wait_send()
    for i in range(1, 8):
        stat_send(i).wait_send()

    def settle(c):
        for at, ev in plans[c]:
            if ev[0] == "send":
                sent(c, *ev[1:]).wait_send()

    each_class(settle)


def body(act, gain1, wqkv, wgate, wout, bias, chain, binder, gain2, wup, wdown):
    vmem = pl.BlockSpec(memory_space=pltpu.VMEM)
    hbm = pl.BlockSpec(memory_space=pl.ANY)
    dma, v = pltpu.SemaphoreType.DMA, pltpu.VMEM
    return pl.pallas_call(
        kernel,
        out_shape=jax.ShapeDtypeStruct((S, ROWS, D), BF),
        in_specs=[vmem, vmem, hbm, hbm, hbm, hbm, vmem, vmem, vmem, hbm, hbm],
        out_specs=vmem,
        scratch_shapes=[
            v((S, 8, ROWS, D), BF), v((S, 2, 8, ROWS, D), BF), v((S, 2, ROWS, D), BF),
            v((D, 3 * D), BF), v((D, D), BF), v((D, D), BF), v((D, 2 * FF), BF), v((FF, D), BF),
            v((H, NQ, NK), BF), v((H, NK, NQ), F32),
            v((D, D), BF), v((D, D), BF), v((D, 1024), BF),
            v((S, H, 128, NQ), BF), v((H // 2, NK, 128), BF), v((H, 64, NK), BF),
            v((2, 2, NK, NQ), F32), v((D, NQ), BF), v((H, NQ), F32),
            v((S, 8, ROWS, D), BF), v((S, 8, ROWS, D), BF),
            v((8, ROWS, 128), BF), v((8, ROWS, 128), BF), v((128, NQ), BF), v((S * ROWS, D), F32),
            dma((6,)), dma((S, 7)), dma((S, 4, 2)), dma((S, 8)), dma((S, 8)), dma((S, 4)),
            dma((S, 2)), dma((S, 2)), dma((S,)), dma((S,)), dma((S, 7)), dma((S, 8)),
            dma((7,)), dma((8,)),
        ],
        compiler_params=pltpu.CompilerParams(
            collective_id=0, has_side_effects=True, vmem_limit_bytes=66_000_000
        ),
        name="block",
    )(
        act, gain1, wqkv, wgate, wout, bias, chain.reshape(32, 128), binder.reshape(32, 128),
        gain2, wup, wdown,
    )


def solution(mesh):
    placed = (
        P(None, ("pb", "ka"), None), P(), P(), P(), P(), P(None, "pb", "ka"), P(), P(), P(), P(), P(),
    )
    return jax.shard_map(
        body, mesh=mesh, in_specs=placed, out_specs=P(None, ("pb", "ka"), None), check_vma=False
    )
```

```python
import math

import jax
import jax.numpy as jnp
from jax import lax
from jax.experimental import pallas as pl
from jax.experimental.pallas import tpu as pltpu
from jax.sharding import PartitionSpec as P

EPS = 1e-5
LOG2E = 1.4426950408889634
MASKED = -1e9 * LOG2E
S, ROWS, D, H, HD = 4, 32, 768, 16, 48
NQ, NK, FF = 256, 512, 1536
QSCALE = LOG2E / math.sqrt(HD)
BF, F32 = jnp.bfloat16, jnp.float32
MESH = pl.DeviceIdType.MESH


def dot(a, b):
    return jnp.dot(a, b, preferred_element_type=F32)


def dot_t(a, b):
    return lax.dot_general(a, b, (((1,), (1,)), ((), ())), preferred_element_type=F32)


def norm(values, gain):
    centred = values - jnp.mean(values, axis=-1, keepdims=True)
    spread = jnp.mean(centred * centred, axis=-1, keepdims=True)
    return centred * lax.rsqrt(spread + EPS) * gain


def eye(n):
    return (
        lax.broadcasted_iota(jnp.int32, (n, n), 0) == lax.broadcasted_iota(jnp.int32, (n, n), 1)
    ).astype(F32).astype(BF)


UP = ((0, 0), (1, 0), (1, 1), (2, 0))
DOWN = ((0, 1), (3, 0), (3, 1), (2, 1))
ROUND = ((0, 0), (0, 1), (1, 0), (3, 0))
DIRECT = ((1, 0), (3, 0), (2, 0), (2, 1))
CLASSES = [(e, r) for e in (1, 0) for r in range(4)]


def slot(dx, dy):
    return UP.index((dx, dy)) if (dx, dy) in UP else 4 + DOWN.index((dx, dy))


def rank(op):
    s, kind = op[1], op[0]
    if kind in ("own", "mate", "far", "relay"):
        return s + ("own", "mate", "far", "relay").index(kind)
    return 10 * s + (op[3] if kind == "z" else (ROUND if kind == "side" else DIRECT).index(op[2:]))


def traffic(occupied=22, latency=56):
    have = {c: {} for c in CLASSES}
    pend, free, log = {}, {}, {c: [] for c in CLASSES}
    for c in CLASSES:
        e, r = c
        ops = {l: [] for l in ("x+", "x-", "y", "o", "z+", "z-")}
        for s in range(S):
            have[c]["q", s, 0, 0] = 0
            ops["y"].append((("own", s), ("q", s, 0, 0)))
            for d in ("x+", "x-"):
                ops[d].append((("own", s), ("q", s, 0, 0)))
                ops[d].append((("mate", s), ("q", s, 0, 1)))
            ops["x+"].append((("far", s), ("q", s, 3, 0)))
            ops["x-"].append((("far", s), ("q", s, 1, 1)))
            for d, owners, end in (("z+", UP, 3), ("z-", DOWN, 1)):
                for g in range(4):
                    if r != end:
                        ops[d].append((("z", s, d, g), ("q" if c == (1, 0) else "k", s) + owners[g]))
            if c == (0, 0):
                ops["o"] += [(("cross", s) + o, ("q", s) + o) for o in DIRECT]
            if c == (1, 0):
                ops["o"] += [(("side", s) + o, ("q", s) + o) for o in ROUND]
                ops["y"] += [(("relay", s) + o, ("rl", s) + o) for o in ROUND]
        pend[c] = ops
        free.update({(c, l): 0 for l in ops})
    for now in range(2000):
        for c in CLASSES:
            e, r = c
            for l, ops in pend[c].items():
                ready = [o for o in ops if have[c].get(o[1], now + 1) <= now]
                if free[c, l] > now or not ready:
                    continue
                o = min(ready, key=lambda o: rank(o[0]))
                ops.remove(o)
                free[c, l] = now + occupied
                op, s = o[0], o[0][1]
                log[c].append((now, op, o[1], l))
                step = {"x+": -1, "x-": 1, "z+": 1, "z-": -1}.get(l, 0)
                to = (1 - e if l == "y" else e, (r + step) % 4)
                if op[0] == "z":
                    item = ("k",) + o[1][1:]
                elif op[0] == "cross":
                    item = ("k",) + op[1:]
                elif op[0] == "side":
                    item = ("rl",) + op[1:]
                elif op[0] == "relay":
                    item = ("k", s, op[2], 1 - op[3])
                elif l == "y":
                    item = ("q", s, 0, 1)
                elif op[0] == "far":
                    item = ("q", s, 2, 0 if l == "x+" else 1)
                else:
                    item = ("q", s, 3 if l == "x+" else 1, 0 if op[0] == "own" else 1)
                assert item not in have[to]
                have[to][item] = now + occupied + latency
    plans = {}
    for c in CLASSES:
        assert not any(pend[c].values())
        events = [(t, ("send",) + tuple(rest)) for t, *rest in log[c]]
        for s in range(S):
            for kind in ("q", "k"):
                items = [(kind, s, dx, dy) for dx in range(4) for dy in range(2)]
                if kind == "k" and c == (1, 0):
                    continue
                at = max(have[c][i] for i in items)
                events.append((at, ("all", kind, s, items)))
                if kind == "k" or c == (1, 0):
                    events.append((at, ("twin", s)))
        events.sort(key=lambda v: v[0])
        waited = {("q", s, 0, 0) for s in range(S)}
        plan = []
        for at, ev in events:
            needs = ev[3] if ev[0] == "all" else [ev[2]] if ev[0] == "send" else []
            for item in needs:
                if item not in waited:
                    waited.add(item)
                    plan.append((at, ("wait", item)))
            if ev[0] != "all":
                plan.append((at, ev))
        plans[c] = plan
    return plans


def kernel(
    act, gain1, wqkv_h, wgate_h, wout_h, bias_h, chain, binder, gain2, wup_h, wdown_h,
    out,
    xq, xk, rl, wqkv, wgate, wout, wup, wdown, bias, bt, wqt, wvt, wkp, qtp, kp, vt,
    st, ot, lse, msg, rbuf, smsg, srbuf, ost, gate,
    wsem, p1s, p1r, zs, zr, crs, rls, rlr, ds, dr, rss, rsr, sss, ssr,
):
    pb, ka = lax.axis_index("pb"), lax.axis_index("ka")
    z, core = pb // 4, pb % 2
    x, ylo = ka // 2, ka % 2
    yhi = (pb // 2) % 2
    r = (z - x + 4) % 4
    same = yhi == ylo
    odd = jnp.where(same, 0, 1)
    xp, xm = (ka + 2) % 8, (ka + 6) % 8
    mate = x * 2 + (1 - ylo)
    zp, zm = (pb + 4) % 16, (pb + 12) % 16
    twin = (pb // 2) * 2 + (1 - core)
    opp = (z * 4 + (1 - yhi) * 2 + core, mate)

    def rcopy(src, dst, ssem, rsem, dev):
        return pltpu.make_async_remote_copy(
            src_ref=src, dst_ref=dst, send_sem=ssem, recv_sem=rsem,
            device_id=dev, device_id_type=MESH,
        )

    local = [
        pltpu.make_async_copy(a, b, wsem.at[i])
        for i, (a, b) in enumerate(
            ((wqkv_h, wqkv), (bias_h, bias), (wgate_h, wgate), (wout_h, wout), (wup_h, wup), (wdown_h, wdown))
        )
    ]
    local[0].start()
    barrier = pltpu.get_barrier_semaphore()
    for i in range(1, 8):
        pl.semaphore_signal(barrier, inc=1, device_id=(pb, (ka + i) % 8), device_id_type=MESH)
    for dev in ((zp, ka), (zm, ka), (twin, ka), opp):
        pl.semaphore_signal(barrier, inc=1, device_id=dev, device_id_type=MESH)

    for s in range(S):
        xq[s, ka] = norm(act[s].astype(F32), gain1[...].reshape(1, D)).astype(BF)

    def q_at(dx, dy):
        return ((x + dx) % 4) * 2 + (ylo + dy) % 2

    def k_at(dx, dy):
        return ((x + dx) % 4) * 2 + (ylo + dy + odd) % 2

    def sent(c, op, item, link):
        kind, s = op[0], op[1]
        if kind in ("own", "mate", "far"):
            ref = xq.at[s, q_at(*item[2:])]
            up = link == "x+"
            if link == "y":
                n, sem, to = 0, (0, 1), mate
            else:
                to = xp if up else xm
                n = {"own": 1, "mate": 3, "far": 5}[kind] + (0 if up else 1)
                if kind == "far":
                    sem = (2, 0 if up else 1)
                else:
                    sem = (3 if up else 1, 0 if kind == "own" else 1)
            return rcopy(ref, ref, p1s.at[s, n], p1r.at[s, sem[0], sem[1]], (pb, to))
        if kind == "z":
            owner = item[2:]
            at = k_at(*owner)
            n = slot(*owner)
            src = xq if item[0] == "q" else xk.at[:, core]
            return rcopy(src.at[s, at], xk.at[s, core, at], zs.at[s, n], zr.at[s, n], (zp if link == "z+" else zm, ka))
        owner, at = item[2:], q_at(*item[2:])
        if kind == "cross":
            n = DIRECT.index(owner)
            return rcopy(xq.at[s, at], xk.at[s, core, at], crs.at[s, n], zr.at[s, slot(*owner)], opp)
        n = ROUND.index(owner)
        if kind == "side":
            return rcopy(xq.at[s, at], rl.at[s, n], crs.at[s, n], rlr.at[s, n], opp)
        dx, dy = owner
        return rcopy(rl.at[s, n], xk.at[s, core, q_at(dx, 1 - dy)], rls.at[s, n], zr.at[s, slot(dx, 1 - dy)], (pb, mate))

    def arrived(item):
        s = item[1]
        if item[0] == "q":
            ref, ssem, rsem = xq.at[s, q_at(*item[2:])], p1s.at[s, 0], p1r.at[s, item[2], item[3]]
        elif item[0] == "k":
            n = slot(*item[2:])
            ref, ssem, rsem = xk.at[s, core, k_at(*item[2:])], zs.at[s, n], zr.at[s, n]
        else:
            n = ROUND.index(item[2:])
            ref, ssem, rsem = rl.at[s, n], rls.at[s, n], rlr.at[s, n]
        rcopy(ref, ref, ssem, rsem, opp).wait_recv()

    def twin_send(s, src):
        return rcopy(src, xk.at[s, core], ds.at[s], dr.at[s], (twin, ka))

    plans = traffic()

    def each_class(body):
        for c in CLASSES:
            @pl.when(jnp.logical_and(odd == 1 - c[0], r == c[1]))
            def _():
                body(c)

    done = [0]

    def until(us):
        low, high = done[0], round(20 * us)
        done[0] = high
        for c in CLASSES:
            events = [ev for at, ev in plans[c] if low <= at < high]
            if not events:
                continue

            @pl.when(jnp.logical_and(odd == 1 - c[0], r == c[1]))
            def _():
                for ev in events:
                    if ev[0] == "wait":
                        arrived(ev[1])
                    elif ev[0] == "send":
                        sent(c, *ev[1:]).start()
                    elif c == (1, 0):
                        twin_send(ev[1], xq.at[ev[1]]).start()
                        xk[ev[1], core] = xq[ev[1]]
                    else:
                        twin_send(ev[1], xk.at[ev[1], core]).start()

    def turn_query_weights():
        local[0].wait()
        e = eye(256)
        for i in range(3):
            wqt[256 * i:256 * i + 256, :] = dot_t(e, wqkv[:, 256 * i:256 * i + 256]).astype(BF)
        qtp[...] = jnp.zeros_like(qtp)

    def turn_value_weights():
        e = eye(256)
        for i in range(3):
            wvt[256 * i:256 * i + 256, :] = dot_t(e, wqkv[:, 2 * D + 256 * i:2 * D + 256 * i + 256]).astype(BF)
        ost[...] = jnp.zeros_like(ost)
        tail = lax.broadcasted_iota(jnp.int32, (16, 16, NK), 1)
        vt[:, HD:64, :] = (tail == 0).astype(F32).astype(BF)

    def pad_key_weights():
        row = lax.broadcasted_iota(jnp.int32, (256, 256), 0)
        col = lax.broadcasted_iota(jnp.int32, (256, 256), 1)
        source = (col // 64) * HD + col % 64
        for t in range(4):
            start, off = (384 * (t // 2), 0) if t % 2 == 0 else (384 * (t // 2) + 128, 64)
            pick = jnp.logical_and(row == source + off, col % 64 < HD).astype(F32).astype(BF)
            wkp[:, 256 * t:256 * t + 256] = dot(wqkv[:, D + start:D + start + 256], pick).astype(BF)

    def prep_bias():
        local[1].wait()
        qc, qb = chain[pl.ds(pb * 2, 2), :], binder[pl.ds(pb * 2, 2), :]
        kc, kb = chain[pl.ds(ka * 4, 4), :], binder[pl.ds(ka * 4, 4), :]

        def features(c, b, n, at):
            c = jnp.concatenate([c[i:i + 1] for i in range(n // 128)], axis=1)
            b = jnp.concatenate([b[i:i + 1] for i in range(n // 128)], axis=1)
            kind = lax.broadcasted_iota(jnp.int32, (16, n), 0)
            f = jnp.where(kind == c, 1.0, 0.0)
            f = jnp.where(kind == 6 + at, jnp.where(b > 0, 1.0, 0.0), f)
            return jnp.where(kind == 7 - at, 1.0, f).astype(BF)

        allow = lax.dot_general(
            features(kc, kb, NK, 1), features(qc, qb, NQ, 0), (((0,), (0,)), ((), ())), preferred_element_type=F32
        )
        st[0, 0] = allow

    def bias_part(i):
        def head(h, carry):
            e = eye(256)
            for t in range(2):
                b = dot_t(e, bias[h, :, 256 * t:256 * t + 256]) * LOG2E
                bt[h, 256 * t:256 * t + 256, :] = jnp.where(st[0, 0, 256 * t:256 * t + 256, :] > 0.5, b, MASKED)
            return carry

        lax.fori_loop(2 * i, 2 * i + 2, head, 0)

    def prep_gate():
        local[2].wait()
        n = xq[:, ka].reshape(S * ROWS, D)
        gate[...] = 1.0 / (1.0 + jnp.exp(-dot(n, wgate[...])))

    def queries(s):
        qs = xq[s].reshape(NQ, D)
        q = (dot_t(wqt[...], qs) * QSCALE).astype(BF)
        for h in range(H):
            off = 64 * (h % 2)
            qtp[s, h, off:off + HD, :] = q[HD * h:HD * h + HD]

    ready = [max(at for p in plans.values() for at, ev in p if ev == ("twin", s)) / 20 + 0.05 for s in range(S)]
    outer = ready[0]
    inner = [ready[i] + (ready[i + 1] - ready[i]) * (n + 1) / 3 for i in range(S - 1) for n in range(3)]
    inner[-1] = 90

    def window(i, n):
        at = 3 * i + n
        done[0] = round(20 * (inner[at - 1] if at else outer))
        until(inner[at])

    def attend(s):
        ks = xk[s].reshape(NK, D)
        for n in range(4):
            k = dot(ks, wkp[:, 256 * n:256 * n + 256]).astype(BF)
            kp[2 * n] = k[:, :128]
            kp[2 * n + 1] = k[:, 128:]
        for t in range(2):
            v = dot_t(wvt[...], ks[256 * t:256 * t + 256]).astype(BF)
            for h in range(H):
                vt[h, 0:HD, 256 * t:256 * t + 256] = v[HD * h:HD * h + HD]

        def scores(hp):
            tops = []
            for j in range(2):
                h = 2 * hp + j
                top = None
                for c in range(4):
                    v = dot(kp[hp, 128 * c:128 * c + 128, :], qtp[s, h]) + bt[h, 128 * c:128 * c + 128, :]
                    st[hp % 2, j, 128 * c:128 * c + 128, :] = v
                    m = jnp.max(v.reshape(16, 8, NQ), axis=0)
                    top = m if top is None else jnp.maximum(top, m)
                tops.append(jnp.max(top, axis=0, keepdims=True))
            return tops

        def weigh(hp, tops):
            for j in range(2):
                h = 2 * hp + j
                w = jnp.exp2(st[hp % 2, j] - tops[j]).astype(BF)
                o = dot(vt[h], w)
                total = o[HD:HD + 1]
                ot[HD * h:HD * h + HD, :] = (o[:HD] * (1.0 / total)).astype(BF)
                lse[h:h + 1, :] = tops[j] + jnp.log2(total)

        tops = scores(0)
        for hp in range(H // 2):
            if hp in (0, 2, 5):
                for i in range(S - 1):
                    @pl.when(s == i)
                    def _():
                        window(i, (0, 2, 5).index(hp))

            later = scores(hp + 1) if hp < H // 2 - 1 else None
            weigh(hp, tops)
            tops = later
        rest = lse[...]
        for i in range(2):
            part = rest.astype(BF)
            ost[pl.ds(pl.multiple_of(32 * s + 16 * i, 16), 16), :] = part
            rest = rest - part.astype(F32)
        e = eye(256)
        for t in range(3):
            lo = 256 * t
            msg[s, :, :, lo:lo + 256] = dot_t(e, ot[lo:lo + 256, :]).astype(BF).reshape(8, ROWS, 256)
        rbuf[s, ka] = msg[s, ka]

    def rs_send(s, i):
        to = (ka + i) % 8
        return rcopy(msg.at[s, to], rbuf.at[s, ka], rss.at[s, i - 1], rsr.at[s, 8 - i], (pb, to))

    def rs_wait(s, i):
        frm = (ka + i) % 8
        rcopy(msg.at[s, frm], rbuf.at[s, frm], rss.at[s, 0], rsr.at[s, i], (pb, frm)).wait_recv()

    def stat_send(i):
        to = (ka + i) % 8
        return rcopy(smsg.at[to], srbuf.at[ka], sss.at[i - 1], ssr.at[8 - i], (pb, to))

    def stat_wait(i):
        frm = (ka + i) % 8
        rcopy(smsg.at[frm], srbuf.at[frm], sss.at[0], ssr.at[i], (pb, frm)).wait_recv()

    def stats():
        smsg[...] = dot_t(eye(256), ost[...]).astype(BF).reshape(8, ROWS, 128)
        srbuf[ka] = smsg[ka]

    def finish():
        lane = lax.broadcasted_iota(jnp.int32, (128, 128), 1)
        row = lax.broadcasted_iota(jnp.int32, (128, 128), 0)
        erow = lax.broadcasted_iota(jnp.int32, (128, D), 0)
        ecol = lax.broadcasted_iota(jnp.int32, (128, D), 1)
        expand = jnp.logical_and(ecol // HD == erow % 16, erow < 32).astype(F32).astype(BF)
        parts = srbuf[...].reshape(8 * ROWS, 128)
        logs = []
        for s in range(S):
            own = jnp.logical_and(row % 16 == lane % 16, row // 32 == s).astype(F32).astype(BF)
            logs.append(dot(parts, own))
        sums = [jnp.concatenate([v[ROWS * b:ROWS * b + ROWS] for v in logs], axis=0) for b in range(8)]
        top = sums[0]
        for b in range(1, 8):
            top = jnp.maximum(top, sums[b])
        w = [jnp.exp2(v - top) for v in sums]
        total = w[0]
        for b in range(1, 8):
            total = total + w[b]
        inv = 1.0 / total
        acc = jnp.zeros((S * ROWS, D), F32)
        for b in range(8):
            v = w[b] * inv
            hi = v.astype(BF)
            low = (v - hi.astype(F32)).astype(BF)
            both = jnp.where(lane < 16, hi.astype(F32), jnp.where(lane < 32, low.astype(F32), 0.0)).astype(BF)
            acc = acc + dot(both, expand) * rbuf[:, b].reshape(S * ROWS, D).astype(F32)
        gated = (gate[...] * acc).astype(BF)
        local[3].wait()
        mixed = act[...].reshape(S * ROWS, D).astype(F32) + dot(gated, wout[...])
        normed = norm(mixed, gain2[...].reshape(1, D)).astype(BF)
        local[4].wait()
        left = dot(normed, wup[:, :FF])
        right = dot(normed, wup[:, FF:])
        hidden = (left / (1.0 + jnp.exp(-left)) * right).astype(BF)
        local[5].wait()
        out[...] = (mixed + dot(hidden, wdown[...])).astype(BF).reshape(S, ROWS, D)

    local[1].start()
    pl.semaphore_wait(barrier, 11)
    until(1)
    turn_query_weights()
    for c in local[2:]:
        c.start()
    until(3.4)
    turn_value_weights()
    until(4)
    pad_key_weights()
    until(5)
    prep_bias()
    until(6)
    for i in range(8):
        bias_part(i)
        until(7 + i)
    queries(0)
    until(15)
    prep_gate()
    until(16)
    queries(1)
    for us in (17, 18, 19, 20):
        until(us)
    queries(2)
    for us in (21, 22, 23):
        until(us)
    until(24)
    queries(3)
    until(25)
    until(outer)

    def step(s, carry):
        twin_recv(s)
        attend(s)
        for i in (4, 3, 5, 2, 6, 1, 7):
            rs_send(s, i).start()
        return carry

    def twin_recv(s):
        rcopy(xk.at[s, 1 - core], xk.at[s, 1 - core], ds.at[s], dr.at[s], (twin, ka)).wait_recv()

    lax.fori_loop(0, S, step, 0)

    stats()
    for i in (4, 3, 5, 2, 6, 1, 7):
        stat_send(i).start()
    for s in range(S):
        for i in range(1, 8):
            rs_wait(s, i)
    for i in range(1, 8):
        stat_wait(i)
    finish()

    for s in range(S):
        for i in range(1, 8):
            rs_send(s, i).wait_send()
        twin_send(s, xq.at[s]).wait_send()
    for i in range(1, 8):
        stat_send(i).wait_send()

    def settle(c):
        for at, ev in plans[c]:
            if ev[0] == "send":
                sent(c, *ev[1:]).wait_send()

    each_class(settle)


def body(act, gain1, wqkv, wgate, wout, bias, chain, binder, gain2, wup, wdown):
    vmem = pl.BlockSpec(memory_space=pltpu.VMEM)
    hbm = pl.BlockSpec(memory_space=pl.ANY)
    dma, v = pltpu.SemaphoreType.DMA, pltpu.VMEM
    return pl.pallas_call(
        kernel,
        out_shape=jax.ShapeDtypeStruct((S, ROWS, D), BF),
        in_specs=[vmem, vmem, hbm, hbm, hbm, hbm, vmem, vmem, vmem, hbm, hbm],
        out_specs=vmem,
        scratch_shapes=[
            v((S, 8, ROWS, D), BF), v((S, 2, 8, ROWS, D), BF), v((S, 4, ROWS, D), BF),
            v((D, 3 * D), BF), v((D, D), BF), v((D, D), BF), v((D, 2 * FF), BF), v((FF, D), BF),
            v((H, NQ, NK), BF), v((H, NK, NQ), F32),
            v((D, D), BF), v((D, D), BF), v((D, 1024), BF),
            v((S, H, 128, NQ), BF), v((H // 2, NK, 128), BF), v((H, 64, NK), BF),
            v((2, 2, NK, NQ), F32), v((D, NQ), BF), v((H, NQ), F32),
            v((S, 8, ROWS, D), BF), v((S, 8, ROWS, D), BF),
            v((8, ROWS, 128), BF), v((8, ROWS, 128), BF), v((128, NQ), BF), v((S * ROWS, D), F32),
            dma((6,)), dma((S, 7)), dma((S, 4, 2)), dma((S, 8)), dma((S, 8)), dma((S, 4)),
            dma((S, 4)), dma((S, 4)), dma((S,)), dma((S,)), dma((S, 7)), dma((S, 8)),
            dma((7,)), dma((8,)),
        ],
        compiler_params=pltpu.CompilerParams(
            collective_id=0, has_side_effects=True, vmem_limit_bytes=66_000_000
        ),
        name="block",
    )(
        act, gain1, wqkv, wgate, wout, bias, chain.reshape(32, 128), binder.reshape(32, 128),
        gain2, wup, wdown,
    )


def solution(mesh):
    placed = (
        P(None, ("pb", "ka"), None), P(), P(), P(), P(), P(None, "pb", "ka"), P(), P(), P(), P(), P(),
    )
    return jax.shard_map(
        body, mesh=mesh, in_specs=placed, out_specs=P(None, ("pb", "ka"), None), check_vma=False
    )
```

```python
import math

import jax
import jax.numpy as jnp
from jax import lax
from jax.experimental import pallas as pl
from jax.experimental.pallas import tpu as pltpu
from jax.sharding import PartitionSpec as P

EPS = 1e-5
LOG2E = 1.4426950408889634
MASKED = -1e9 * LOG2E
S, ROWS, D, H, HD = 4, 32, 768, 16, 48
NQ, NK, FF = 256, 512, 1536
QSCALE = LOG2E / math.sqrt(HD)
BF, F32 = jnp.bfloat16, jnp.float32
MESH = pl.DeviceIdType.MESH


def dot(a, b):
    return jnp.dot(a, b, preferred_element_type=F32)


def dot_t(a, b):
    return lax.dot_general(a, b, (((1,), (1,)), ((), ())), preferred_element_type=F32)


def norm(values, gain):
    centred = values - jnp.mean(values, axis=-1, keepdims=True)
    spread = jnp.mean(centred * centred, axis=-1, keepdims=True)
    return centred * lax.rsqrt(spread + EPS) * gain


def eye(n):
    return (
        lax.broadcasted_iota(jnp.int32, (n, n), 0) == lax.broadcasted_iota(jnp.int32, (n, n), 1)
    ).astype(F32).astype(BF)


UP = ((0, 0), (1, 0), (1, 1), (2, 0))
DOWN = ((0, 1), (3, 0), (3, 1), (2, 1))
ROUND = ((0, 0), (0, 1), (1, 0), (3, 0))
DIRECT = ((1, 0), (3, 0), (2, 0), (2, 1))
CLASSES = [(e, r) for e in (1, 0) for r in range(4)]


def slot(dx, dy):
    return UP.index((dx, dy)) if (dx, dy) in UP else 4 + DOWN.index((dx, dy))


def rank(op):
    s, kind = op[1], op[0]
    if kind in ("own", "mate", "far", "relay"):
        return s + ("own", "mate", "far", "relay").index(kind)
    return 10 * s + (op[3] if kind == "z" else (ROUND if kind == "side" else DIRECT).index(op[2:]))


def traffic(occupied=22, latency=56):
    have = {c: {} for c in CLASSES}
    pend, free, log = {}, {}, {c: [] for c in CLASSES}
    for c in CLASSES:
        e, r = c
        ops = {l: [] for l in ("x+", "x-", "y", "o", "z+", "z-")}
        for s in range(S):
            have[c]["q", s, 0, 0] = 0
            ops["y"].append((("own", s), ("q", s, 0, 0)))
            for d in ("x+", "x-"):
                ops[d].append((("own", s), ("q", s, 0, 0)))
                ops[d].append((("mate", s), ("q", s, 0, 1)))
            ops["x+"].append((("far", s), ("q", s, 3, 0)))
            ops["x-"].append((("far", s), ("q", s, 1, 1)))
            for d, owners, end in (("z+", UP, 3), ("z-", DOWN, 1)):
                for g in range(4):
                    if r != end:
                        ops[d].append((("z", s, d, g), ("q" if c == (1, 0) else "k", s) + owners[g]))
            if c == (0, 0):
                ops["o"] += [(("cross", s) + o, ("q", s) + o) for o in DIRECT]
            if c == (1, 0):
                ops["o"] += [(("side", s) + o, ("q", s) + o) for o in ROUND]
                ops["y"] += [(("relay", s) + o, ("rl", s) + o) for o in ROUND]
        pend[c] = ops
        free.update({(c, l): 0 for l in ops})
    for now in range(2000):
        for c in CLASSES:
            e, r = c
            for l, ops in pend[c].items():
                ready = [o for o in ops if have[c].get(o[1], now + 1) <= now]
                if free[c, l] > now or not ready:
                    continue
                o = min(ready, key=lambda o: rank(o[0]))
                ops.remove(o)
                free[c, l] = now + occupied
                op, s = o[0], o[0][1]
                log[c].append((now, op, o[1], l))
                step = {"x+": -1, "x-": 1, "z+": 1, "z-": -1}.get(l, 0)
                to = (1 - e if l == "y" else e, (r + step) % 4)
                if op[0] == "z":
                    item = ("k",) + o[1][1:]
                elif op[0] == "cross":
                    item = ("k",) + op[1:]
                elif op[0] == "side":
                    item = ("rl",) + op[1:]
                elif op[0] == "relay":
                    item = ("k", s, op[2], 1 - op[3])
                elif l == "y":
                    item = ("q", s, 0, 1)
                elif op[0] == "far":
                    item = ("q", s, 2, 0 if l == "x+" else 1)
                else:
                    item = ("q", s, 3 if l == "x+" else 1, 0 if op[0] == "own" else 1)
                assert item not in have[to]
                have[to][item] = now + occupied + latency
    plans = {}
    for c in CLASSES:
        assert not any(pend[c].values())
        events = [(t, ("send",) + tuple(rest)) for t, *rest in log[c]]
        for s in range(S):
            for kind in ("q", "k"):
                items = [(kind, s, dx, dy) for dx in range(4) for dy in range(2)]
                if kind == "k" and c == (1, 0):
                    continue
                at = max(have[c][i] for i in items)
                events.append((at, ("all", kind, s, items)))
                if kind == "k" or c == (1, 0):
                    events.append((at, ("twin", s)))
        events.sort(key=lambda v: v[0])
        waited = {("q", s, 0, 0) for s in range(S)}
        plan = []
        for at, ev in events:
            needs = ev[3] if ev[0] == "all" else [ev[2]] if ev[0] == "send" else []
            for item in needs:
                if item not in waited:
                    waited.add(item)
                    plan.append((at, ("wait", item)))
            if ev[0] != "all":
                plan.append((at, ev))
        plans[c] = plan
    return plans


def kernel(
    act, gain1, wqkv_h, wgate_h, wout_h, bias_h, chain, binder, gain2, wup_h, wdown_h,
    out,
    xq, xk, rl, wqkv, wgate, wout, wup, wdown, bias, bt, wqt, wvt, wkp, qtp, kp, vt,
    st, ot, lse, msg, rbuf, smsg, srbuf, ost, gate,
    wsem, p1s, p1r, zs, zr, crs, rls, rlr, ds, dr, rss, rsr, sss, ssr,
):
    pb, ka = lax.axis_index("pb"), lax.axis_index("ka")
    z, core = pb // 4, pb % 2
    x, ylo = ka // 2, ka % 2
    yhi = (pb // 2) % 2
    r = (z - x + 4) % 4
    same = yhi == ylo
    odd = jnp.where(same, 0, 1)
    xp, xm = (ka + 2) % 8, (ka + 6) % 8
    mate = x * 2 + (1 - ylo)
    zp, zm = (pb + 4) % 16, (pb + 12) % 16
    twin = (pb // 2) * 2 + (1 - core)
    opp = (z * 4 + (1 - yhi) * 2 + core, mate)

    def rcopy(src, dst, ssem, rsem, dev):
        return pltpu.make_async_remote_copy(
            src_ref=src, dst_ref=dst, send_sem=ssem, recv_sem=rsem,
            device_id=dev, device_id_type=MESH,
        )

    local = [
        pltpu.make_async_copy(a, b, wsem.at[i])
        for i, (a, b) in enumerate(
            ((wqkv_h, wqkv), (bias_h, bias), (wgate_h, wgate), (wout_h, wout), (wup_h, wup), (wdown_h, wdown))
        )
    ]
    local[0].start()
    barrier = pltpu.get_barrier_semaphore()
    for i in range(1, 8):
        pl.semaphore_signal(barrier, inc=1, device_id=(pb, (ka + i) % 8), device_id_type=MESH)
    for dev in ((zp, ka), (zm, ka), (twin, ka), opp):
        pl.semaphore_signal(barrier, inc=1, device_id=dev, device_id_type=MESH)

    for s in range(S):
        xq[s, ka] = norm(act[s].astype(F32), gain1[...].reshape(1, D)).astype(BF)

    def q_at(dx, dy):
        return ((x + dx) % 4) * 2 + (ylo + dy) % 2

    def k_at(dx, dy):
        return ((x + dx) % 4) * 2 + (ylo + dy + odd) % 2

    def sent(c, op, item, link):
        kind, s = op[0], op[1]
        if kind in ("own", "mate", "far"):
            ref = xq.at[s, q_at(*item[2:])]
            up = link == "x+"
            if link == "y":
                n, sem, to = 0, (0, 1), mate
            else:
                to = xp if up else xm
                n = {"own": 1, "mate": 3, "far": 5}[kind] + (0 if up else 1)
                if kind == "far":
                    sem = (2, 0 if up else 1)
                else:
                    sem = (3 if up else 1, 0 if kind == "own" else 1)
            return rcopy(ref, ref, p1s.at[s, n], p1r.at[s, sem[0], sem[1]], (pb, to))
        if kind == "z":
            owner = item[2:]
            at = k_at(*owner)
            n = slot(*owner)
            src = xq if item[0] == "q" else xk.at[:, core]
            return rcopy(src.at[s, at], xk.at[s, core, at], zs.at[s, n], zr.at[s, n], (zp if link == "z+" else zm, ka))
        owner, at = item[2:], q_at(*item[2:])
        if kind == "cross":
            n = DIRECT.index(owner)
            return rcopy(xq.at[s, at], xk.at[s, core, at], crs.at[s, n], zr.at[s, slot(*owner)], opp)
        n = ROUND.index(owner)
        if kind == "side":
            return rcopy(xq.at[s, at], rl.at[s, n], crs.at[s, n], rlr.at[s, n], opp)
        dx, dy = owner
        return rcopy(rl.at[s, n], xk.at[s, core, q_at(dx, 1 - dy)], rls.at[s, n], zr.at[s, slot(dx, 1 - dy)], (pb, mate))

    def arrived(item):
        s = item[1]
        if item[0] == "q":
            ref, ssem, rsem = xq.at[s, q_at(*item[2:])], p1s.at[s, 0], p1r.at[s, item[2], item[3]]
        elif item[0] == "k":
            n = slot(*item[2:])
            ref, ssem, rsem = xk.at[s, core, k_at(*item[2:])], zs.at[s, n], zr.at[s, n]
        else:
            n = ROUND.index(item[2:])
            ref, ssem, rsem = rl.at[s, n], rls.at[s, n], rlr.at[s, n]
        rcopy(ref, ref, ssem, rsem, opp).wait_recv()

    def twin_send(s, src):
        return rcopy(src, xk.at[s, core], ds.at[s], dr.at[s], (twin, ka))

    plans = traffic()

    def each_class(body):
        for c in CLASSES:
            @pl.when(jnp.logical_and(odd == 1 - c[0], r == c[1]))
            def _():
                body(c)

    done = [0]

    def until(us):
        low, high = done[0], round(20 * us)
        done[0] = high
        for c in CLASSES:
            events = [ev for at, ev in plans[c] if low <= at < high]
            if not events:
                continue

            @pl.when(jnp.logical_and(odd == 1 - c[0], r == c[1]))
            def _():
                for ev in events:
                    if ev[0] == "wait":
                        arrived(ev[1])
                    elif ev[0] == "send":
                        sent(c, *ev[1:]).start()
                    elif c == (1, 0):
                        twin_send(ev[1], xq.at[ev[1]]).start()
                        xk[ev[1], core] = xq[ev[1]]
                    else:
                        twin_send(ev[1], xk.at[ev[1], core]).start()

    def turn_query_weights():
        local[0].wait()
        e = eye(256)
        for i in range(3):
            wqt[256 * i:256 * i + 256, :] = dot_t(e, wqkv[:, 256 * i:256 * i + 256]).astype(BF)
        qtp[...] = jnp.zeros_like(qtp)

    def turn_value_weights():
        e = eye(256)
        for i in range(3):
            wvt[256 * i:256 * i + 256, :] = dot_t(e, wqkv[:, 2 * D + 256 * i:2 * D + 256 * i + 256]).astype(BF)
        ost[...] = jnp.zeros_like(ost)
        tail = lax.broadcasted_iota(jnp.int32, (16, 16, NK), 1)
        vt[:, HD:64, :] = (tail == 0).astype(F32).astype(BF)

    def pad_key_weights():
        row = lax.broadcasted_iota(jnp.int32, (256, 256), 0)
        col = lax.broadcasted_iota(jnp.int32, (256, 256), 1)
        source = (col // 64) * HD + col % 64
        for t in range(4):
            start, off = (384 * (t // 2), 0) if t % 2 == 0 else (384 * (t // 2) + 128, 64)
            pick = jnp.logical_and(row == source + off, col % 64 < HD).astype(F32).astype(BF)
            wkp[:, 256 * t:256 * t + 256] = dot(wqkv[:, D + start:D + start + 256], pick).astype(BF)

    def prep_bias():
        local[1].wait()
        qc, qb = chain[pl.ds(pb * 2, 2), :], binder[pl.ds(pb * 2, 2), :]
        kc, kb = chain[pl.ds(ka * 4, 4), :], binder[pl.ds(ka * 4, 4), :]

        def features(c, b, n, at):
            c = jnp.concatenate([c[i:i + 1] for i in range(n // 128)], axis=1)
            b = jnp.concatenate([b[i:i + 1] for i in range(n // 128)], axis=1)
            kind = lax.broadcasted_iota(jnp.int32, (16, n), 0)
            f = jnp.where(kind == c, 1.0, 0.0)
            f = jnp.where(kind == 6 + at, jnp.where(b > 0, 1.0, 0.0), f)
            return jnp.where(kind == 7 - at, 1.0, f).astype(BF)

        allow = lax.dot_general(
            features(kc, kb, NK, 1), features(qc, qb, NQ, 0), (((0,), (0,)), ((), ())), preferred_element_type=F32
        )
        st[0, 0] = allow

    def bias_part(i):
        def head(h, carry):
            e = eye(256)
            for t in range(2):
                b = dot_t(e, bias[h, :, 256 * t:256 * t + 256]) * LOG2E
                bt[h, 256 * t:256 * t + 256, :] = jnp.where(st[0, 0, 256 * t:256 * t + 256, :] > 0.5, b, MASKED)
            return carry

        lax.fori_loop(2 * i, 2 * i + 2, head, 0)

    def prep_gate():
        local[2].wait()
        n = xq[:, ka].reshape(S * ROWS, D)
        gate[...] = 1.0 / (1.0 + jnp.exp(-dot(n, wgate[...])))

    def queries(s):
        qs = xq[s].reshape(NQ, D)
        q = (dot_t(wqt[...], qs) * QSCALE).astype(BF)
        for h in range(H):
            off = 64 * (h % 2)
            qtp[s, h, off:off + HD, :] = q[HD * h:HD * h + HD]

    ready = [max(at for p in plans.values() for at, ev in p if ev == ("twin", s)) / 20 + 0.05 for s in range(S)]
    outer = ready[0]
    inner = [ready[i] + (ready[i + 1] - ready[i]) * (n + 1) / 2 for i in range(S - 1) for n in range(2)]
    inner[-1] = 90

    def window(i, n):
        at = 2 * i + n
        done[0] = round(20 * (inner[at - 1] if at else outer))
        until(inner[at])

    def attend(s):
        ks = xk[s].reshape(NK, D)
        for n in range(4):
            k = dot(ks, wkp[:, 256 * n:256 * n + 256]).astype(BF)
            kp[2 * n] = k[:, :128]
            kp[2 * n + 1] = k[:, 128:]
        for t in range(2):
            v = dot_t(wvt[...], ks[256 * t:256 * t + 256]).astype(BF)
            for h in range(H):
                vt[h, 0:HD, 256 * t:256 * t + 256] = v[HD * h:HD * h + HD]

        def scores(hp):
            tops = []
            for j in range(2):
                h = 2 * hp + j
                top = None
                for c in range(4):
                    v = dot(kp[hp, 128 * c:128 * c + 128, :], qtp[s, h]) + bt[h, 128 * c:128 * c + 128, :]
                    st[hp % 2, j, 128 * c:128 * c + 128, :] = v
                    m = jnp.max(v.reshape(16, 8, NQ), axis=0)
                    top = m if top is None else jnp.maximum(top, m)
                tops.append(jnp.max(top, axis=0, keepdims=True))
            return tops

        def weigh(hp, tops):
            for j in range(2):
                h = 2 * hp + j
                w = jnp.exp2(st[hp % 2, j] - tops[j]).astype(BF)
                o = dot(vt[h], w)
                total = o[HD:HD + 1]
                ot[HD * h:HD * h + HD, :] = (o[:HD] * (1.0 / total)).astype(BF)
                lse[h:h + 1, :] = tops[j] + jnp.log2(total)

        tops = scores(0)
        for hp in range(H // 2):
            if hp in (0, 4):
                for i in range(S - 1):
                    @pl.when(s == i)
                    def _():
                        window(i, (0, 4).index(hp))

            later = scores(hp + 1) if hp < H // 2 - 1 else None
            weigh(hp, tops)
            tops = later
        rest = lse[...]
        for i in range(2):
            part = rest.astype(BF)
            ost[pl.ds(pl.multiple_of(32 * s + 16 * i, 16), 16), :] = part
            rest = rest - part.astype(F32)
        e = eye(256)
        for t in range(3):
            lo = 256 * t
            msg[s, :, :, lo:lo + 256] = dot_t(e, ot[lo:lo + 256, :]).astype(BF).reshape(8, ROWS, 256)
        rbuf[s, ka] = msg[s, ka]

    def rs_send(s, i):
        to = (ka + i) % 8
        return rcopy(msg.at[s, to], rbuf.at[s, ka], rss.at[s, i - 1], rsr.at[s, 8 - i], (pb, to))

    def rs_wait(s, i):
        frm = (ka + i) % 8
        rcopy(msg.at[s, frm], rbuf.at[s, frm], rss.at[s, 0], rsr.at[s, i], (pb, frm)).wait_recv()

    def stat_send(i):
        to = (ka + i) % 8
        return rcopy(smsg.at[to], srbuf.at[ka], sss.at[i - 1], ssr.at[8 - i], (pb, to))

    def stat_wait(i):
        frm = (ka + i) % 8
        rcopy(smsg.at[frm], srbuf.at[frm], sss.at[0], ssr.at[i], (pb, frm)).wait_recv()

    def stats():
        smsg[...] = dot_t(eye(256), ost[...]).astype(BF).reshape(8, ROWS, 128)
        srbuf[ka] = smsg[ka]

    def finish():
        lane = lax.broadcasted_iota(jnp.int32, (128, 128), 1)
        row = lax.broadcasted_iota(jnp.int32, (128, 128), 0)
        erow = lax.broadcasted_iota(jnp.int32, (128, D), 0)
        ecol = lax.broadcasted_iota(jnp.int32, (128, D), 1)
        expand = jnp.logical_and(ecol // HD == erow % 16, erow < 32).astype(F32).astype(BF)
        parts = srbuf[...].reshape(8 * ROWS, 128)
        logs = []
        for s in range(S):
            own = jnp.logical_and(row % 16 == lane % 16, row // 32 == s).astype(F32).astype(BF)
            logs.append(dot(parts, own))
        sums = [jnp.concatenate([v[ROWS * b:ROWS * b + ROWS] for v in logs], axis=0) for b in range(8)]
        top = sums[0]
        for b in range(1, 8):
            top = jnp.maximum(top, sums[b])
        w = [jnp.exp2(v - top) for v in sums]
        total = w[0]
        for b in range(1, 8):
            total = total + w[b]
        inv = 1.0 / total
        acc = jnp.zeros((S * ROWS, D), F32)
        for b in range(8):
            v = w[b] * inv
            hi = v.astype(BF)
            low = (v - hi.astype(F32)).astype(BF)
            both = jnp.where(lane < 16, hi.astype(F32), jnp.where(lane < 32, low.astype(F32), 0.0)).astype(BF)
            acc = acc + dot(both, expand) * rbuf[:, b].reshape(S * ROWS, D).astype(F32)
        gated = (gate[...] * acc).astype(BF)
        local[3].wait()
        mixed = act[...].reshape(S * ROWS, D).astype(F32) + dot(gated, wout[...])
        normed = norm(mixed, gain2[...].reshape(1, D)).astype(BF)
        local[4].wait()
        left = dot(normed, wup[:, :FF])
        right = dot(normed, wup[:, FF:])
        hidden = (left / (1.0 + jnp.exp(-left)) * right).astype(BF)
        local[5].wait()
        out[...] = (mixed + dot(hidden, wdown[...])).astype(BF).reshape(S, ROWS, D)

    local[1].start()
    pl.semaphore_wait(barrier, 11)
    until(1)
    turn_query_weights()
    for c in local[2:]:
        c.start()
    until(3.4)
    turn_value_weights()
    until(4)
    pad_key_weights()
    until(5)
    prep_bias()
    until(6)
    for i in range(8):
        bias_part(i)
        until(7 + i)
    queries(0)
    until(15)
    prep_gate()
    until(16)
    queries(1)
    for us in (17, 18, 19, 20):
        until(us)
    queries(2)
    for us in (21, 22, 23):
        until(us)
    until(24)
    queries(3)
    until(25)
    until(outer)

    def step(s, carry):
        twin_recv(s)
        attend(s)
        for i in (4, 3, 5, 2, 6, 1, 7):
            rs_send(s, i).start()
        return carry

    def twin_recv(s):
        rcopy(xk.at[s, 1 - core], xk.at[s, 1 - core], ds.at[s], dr.at[s], (twin, ka)).wait_recv()

    lax.fori_loop(0, S, step, 0)

    stats()
    for i in (4, 3, 5, 2, 6, 1, 7):
        stat_send(i).start()
    for s in range(S):
        for i in range(1, 8):
            rs_wait(s, i)
    for i in range(1, 8):
        stat_wait(i)
    finish()

    for s in range(S):
        for i in range(1, 8):
            rs_send(s, i).wait_send()
        twin_send(s, xq.at[s]).wait_send()
    for i in range(1, 8):
        stat_send(i).wait_send()

    def settle(c):
        for at, ev in plans[c]:
            if ev[0] == "send":
                sent(c, *ev[1:]).wait_send()

    each_class(settle)


def body(act, gain1, wqkv, wgate, wout, bias, chain, binder, gain2, wup, wdown):
    vmem = pl.BlockSpec(memory_space=pltpu.VMEM)
    hbm = pl.BlockSpec(memory_space=pl.ANY)
    dma, v = pltpu.SemaphoreType.DMA, pltpu.VMEM
    return pl.pallas_call(
        kernel,
        out_shape=jax.ShapeDtypeStruct((S, ROWS, D), BF),
        in_specs=[vmem, vmem, hbm, hbm, hbm, hbm, vmem, vmem, vmem, hbm, hbm],
        out_specs=vmem,
        scratch_shapes=[
            v((S, 8, ROWS, D), BF), v((S, 2, 8, ROWS, D), BF), v((S, 4, ROWS, D), BF),
            v((D, 3 * D), BF), v((D, D), BF), v((D, D), BF), v((D, 2 * FF), BF), v((FF, D), BF),
            v((H, NQ, NK), BF), v((H, NK, NQ), F32),
            v((D, D), BF), v((D, D), BF), v((D, 1024), BF),
            v((S, H, 128, NQ), BF), v((H // 2, NK, 128), BF), v((H, 64, NK), BF),
            v((2, 2, NK, NQ), F32), v((D, NQ), BF), v((H, NQ), F32),
            v((S, 8, ROWS, D), BF), v((S, 8, ROWS, D), BF),
            v((8, ROWS, 128), BF), v((8, ROWS, 128), BF), v((128, NQ), BF), v((S * ROWS, D), F32),
            dma((6,)), dma((S, 7)), dma((S, 4, 2)), dma((S, 8)), dma((S, 8)), dma((S, 4)),
            dma((S, 4)), dma((S, 4)), dma((S,)), dma((S,)), dma((S, 7)), dma((S, 8)),
            dma((7,)), dma((8,)),
        ],
        compiler_params=pltpu.CompilerParams(
            collective_id=0, has_side_effects=True, vmem_limit_bytes=66_000_000
        ),
        name="block",
    )(
        act, gain1, wqkv, wgate, wout, bias, chain.reshape(32, 128), binder.reshape(32, 128),
        gain2, wup, wdown,
    )


def solution(mesh):
    placed = (
        P(None, ("pb", "ka"), None), P(), P(), P(), P(), P(None, "pb", "ka"), P(), P(), P(), P(), P(),
    )
    return jax.shard_map(
        body, mesh=mesh, in_specs=placed, out_specs=P(None, ("pb", "ka"), None), check_vma=False
    )
```
